128 devices in a mesh: fit: 8 (over z, core), pair: 16 (over x, y).
Axes of the slice: x: 4, y: 4, z: 4, core: 2. Of those that a mesh axis runs over, the one named last changes fastest.
Arguments:
- metric_factor: bfloat16 [4096, 4096], P('fit'), as said below
- three_index: bfloat16 [4096, 32768], P('fit', 'pair'), may hold values from -6 to 6
- send_map: int32 [16, 16, 8], P('pair'), may hold values from 0 to 15
- pair_slots: int32 [16, 128], P('pair'), may hold values from 0 to 127, each once within a row
- pair_count: int32 [16], P('pair'), may hold values from 1 to 64, 512 in all
- orbital_energy: bfloat16 [256], P('pair'), may hold values from -2 to -0.19921875
- cabs_energy: float32 [1024], replicated, may hold values from 0.5 to 4
- coupling: bfloat16 [128, 1024], replicated, may hold values from -0.5 to 0.5
Outputs:
- projected: bfloat16 [16, 64, 128, 1024], P('pair', 'fit')
The draws below stay inside these ranges and needn't reach their ends.
Inputs may be any that keep to these rules, and one draw needn't show every extreme that they name: `metric_factor`: diagonal entries lie between 0.6 and 1.4. `pair_slots`: each row holds every position 0 to 127 once; pair n of a row uses entries 2n and 2n + 1.
All inputs are finite; a program needn't handle non-finite values. No bound on the sum of `pair_count` on one device may be relied on, other than what follows from the above.
Results may differ from the reference program's by a relative error of at most 0.015.
Values may be sent and summed in bfloat16 or wider, within the bound.
A program may use at most 256 MiB of HBM per device.

```python
import math
import jax
import jax.numpy as jnp
import numpy as np
from jax import lax

NAUX = 4096
DOM = 128
NCABS = 1024
LMO_DEV = 16
PAIR_CAP = 64
NLMO = 256
CAP = 8
N_PAIR = 16


def draw_metric_factor(key, part):
    first, second = jax.random.split(jax.random.fold_in(key, 17))
    spread = jax.random.normal(first, (NAUX, NAUX), jnp.float32) * (0.8 / NAUX ** 0.5)
    diagonal = jax.random.uniform(second, (NAUX,), jnp.float32, 0.6, 1.4)
    eye = jnp.eye(NAUX, dtype=jnp.float32)
    factor = spread * (1.0 - eye) + jnp.diag(diagonal)
    return factor.astype(jnp.bfloat16)


def plant(drawn, stream_key, smallest, largest):
    extent = drawn.shape
    place = [jax.random.randint(jax.random.fold_in(stream_key, axis), (), 0, extent[axis]) for axis in range(len(extent))]
    drawn = drawn.at[tuple(place)].set(smallest)
    longest = extent.index(max(extent))
    place[longest] = (place[longest] + 1) % extent[longest]
    return drawn.at[tuple(place)].set(largest)


def shard_levels(rng, shape, pieces, least, high):
    def one(axis_at, blocks):
        draws = jax.random.uniform(jax.random.fold_in(jax.random.fold_in(rng, 6), axis_at), (blocks,), jnp.float32, least / len(pieces), high / len(pieces))
        return jnp.repeat(jnp.exp(draws), shape[axis_at] // blocks).reshape((-1,) + (1,) * (len(shape) - axis_at - 1))

    loudness = one(*pieces[0])
    for cut in pieces[1:]:
        loudness = loudness * one(*cut)
    return loudness


def split_up(number_of, total, limit, lean):
    portions = [(1 << 20) // math.isqrt(rank ** lean) + 1 for rank in range(2, number_of + 1)]
    spare, counts = total - limit - (number_of - 1), [1] * (number_of - 1)
    while spare > 0:
        movable = [i for i in range(number_of - 1) if counts[i] < limit]
        whole, remaining = sum([portions[i] for i in movable]), spare
        for i in movable:
            addition = min(limit - counts[i], max(1, remaining * portions[i] // whole), spare)
            counts[i] = counts[i] + addition
            spare = spare - addition
    return np.array([limit] + counts)


def ragged_sizes(stream_key, amount, total, limit, lean):
    if amount == 2:
        one = jax.random.randint(stream_key, (), max(1, total - limit), min(limit, total - 1) + 1)
        return jnp.stack([one, total - one])
    sizes = jnp.asarray(split_up(amount, total, limit, lean), jnp.int32)
    pairs = (amount - 1) // 2
    giver, sink = sizes[1:1 + 2 * pairs:2], sizes[2:2 + 2 * pairs:2]
    room = jnp.minimum(giver - 1, limit - sink)
    shifted = jax.random.randint(jax.random.fold_in(stream_key, 1), (pairs,), 0, 1 << 20) % (room + 1)
    sizes = sizes.at[1:1 + 2 * pairs:2].set(giver - shifted).at[2:2 + 2 * pairs:2].set(sink + shifted)
    return sizes[jax.random.permutation(jax.random.fold_in(stream_key, 2), amount)]


def scatter_about(own_key, extent, width, bound, cuts=(), kind=jnp.bfloat16):
    factor_of = shard_levels(own_key, extent, cuts, -0.22, 0.18) if cuts else 1.0
    values = jax.random.normal(own_key, extent, jnp.float32) * width * factor_of
    return jnp.minimum(jnp.maximum(values, -bound), bound).astype(kind)


def setup_inputs(seed: int = 0) -> dict:
    key_of = jax.random.split(jax.random.key(seed), 9)
    metric_factor = draw_metric_factor(jax.random.fold_in(key_of[8], 71), 0)
    three_index = scatter_about(key_of[1], (NAUX, NLMO * DOM), 1.0, 6.0, ((0, 8), (1, 16)))
    send_map = plant(jax.random.randint(key_of[2], (N_PAIR, N_PAIR, CAP), 0, LMO_DEV), jax.random.fold_in(key_of[2], 1), 0, LMO_DEV - 1).astype(jnp.int32)
    pair_slots = jax.vmap(lambda own: jax.random.permutation(own, 2 * PAIR_CAP))(jax.random.split(key_of[3], N_PAIR)).reshape((N_PAIR, 2 * PAIR_CAP)).astype(jnp.int32)
    pair_count = ragged_sizes(key_of[4], N_PAIR, PAIR_CAP * N_PAIR // 2, PAIR_CAP, 2).astype(jnp.int32)
    orbital_energy = jnp.clip(-2.0 + 1.8007812 * jax.random.uniform(key_of[5], (NLMO,), jnp.float32) ** shard_levels(key_of[5], (NLMO,), ((0, 16),), -0.2, 0.2), -2.0, -0.19921875).astype(jnp.bfloat16)
    cabs_energy = jnp.clip(jnp.exp(jax.random.uniform(key_of[6], (NCABS,), jnp.float32, math.log(0.5), math.log(4.0))), 0.5, 4.0)
    coupling = scatter_about(key_of[7], (DOM, NCABS), DOM ** -0.5, 0.5)
    return {"metric_factor": metric_factor, "three_index": three_index, "send_map": send_map, "pair_slots": pair_slots, "pair_count": pair_count, "orbital_energy": orbital_energy, "cabs_energy": cabs_energy, "coupling": coupling}


def reference(metric_factor, three_index, send_map, pair_slots, pair_count, orbital_energy, cabs_energy, coupling):
    fitted = jnp.dot(metric_factor, three_index, preferred_element_type=jnp.float32).astype(jnp.bfloat16)
    fitted = fitted.reshape(NAUX, NLMO, DOM)
    norm_scale = NAUX ** -0.5
    energy = orbital_energy.astype(jnp.float32)
    coupling_wide = coupling.astype(jnp.float32)

    def owner(packed):
        wanted, slots, live_count = packed
        sources = jnp.arange(N_PAIR, dtype=jnp.int32)[:, None] * LMO_DEV
        ident = (sources + wanted).reshape(-1).astype(jnp.int32)
        orbits = ident[slots]
        left_ids = orbits[0::2]
        right_ids = orbits[1::2]
        left_rows = fitted[:, left_ids, :].astype(jnp.float32)
        right_rows = fitted[:, right_ids, :].astype(jnp.float32)
        exchange = jnp.einsum("qsa,qsb->sab", left_rows, right_rows) * norm_scale
        rounded = lax.optimization_barrier(exchange.astype(jnp.bfloat16)).astype(jnp.float32)
        weighted = jnp.einsum("sab,bc->sac", rounded, coupling_wide)
        denom = cabs_energy[None, None, :] - (energy[left_ids] + energy[right_ids])[:, None, None]
        live_mask = jnp.arange(PAIR_CAP, dtype=jnp.int32) < live_count
        return jnp.where(live_mask[:, None, None], weighted / denom, 0.0).astype(jnp.bfloat16)

    return lax.map(owner, (send_map, pair_slots, pair_count))
```

```python
import jax
import jax.numpy as jnp
from jax import lax
from jax.experimental import pallas as pl
from jax.experimental.pallas import tpu as pltpu
from jax.sharding import PartitionSpec as P

MESH = pl.DeviceIdType.MESH
F32 = jnp.float32
BF16 = jnp.bfloat16
CHUNKS = 8
LANES = 128
PANEL = 512
QROWS = 256
SCALE = 4096.0 ** -0.5


def fused_kernel(
    fac, tri, ints, ens, cabs,
    exch_out, rec_out,
    a_v, b_v, f_v, cols, part, rs1, summed, rs2, ints_v, ens_v, ints_s, ens_s,
    a_sem, zs, zr, xs, xr, ys, yr, ps, pr, i_sem, e_sem, r_sem, l_sem,
):
    f = lax.axis_index("fit")
    p = lax.axis_index("pair")
    z, c = f // 2, f % 2
    x, y = p // 4, p % 4
    nc = 1 - c
    zp, zm, zo = (z + 1) % 4, (z + 3) % 4, (z + 2) % 4
    yp, ym, yo = (y + 1) % 4, (y + 3) % 4, (y + 2) % 4

    def dev(zz, cc, xx, yy):
        return (2 * zz + cc, 4 * xx + yy)

    me_partner = dev(z, nc, x, y)

    def remote(src, dst, ss, rs, to):
        return pltpu.make_async_remote_copy(
            src_ref=src, dst_ref=dst, send_sem=ss, recv_sem=rs, device_id=to, device_id_type=MESH
        )

    barrier = pltpu.get_barrier_semaphore()
    greeted = [me_partner]
    for d in (1, 2, 3):
        greeted.append(dev((z + d) % 4, c, x, y))
        greeted.append(dev(z, c, (x + d) % 4, y))
        greeted.append(dev(z, c, x, (y + d) % 4))
    greeted.append(dev(zp, nc, x, y))
    greeted.append(dev(zm, nc, x, y))
    for to in greeted:
        pl.semaphore_signal(barrier, inc=1, device_id=to, device_id_type=MESH)
    pl.semaphore_wait(barrier, len(greeted))

    def own_src(h, g):
        return tri.at[:, pl.ds(pl.multiple_of((h * CHUNKS + g) * LANES, LANES), LANES)]

    def panel(g, k):
        return b_v.at[g, pl.ds(pl.multiple_of(k * PANEL, PANEL), PANEL), :]

    def own_copies(g):
        out = []
        for i, (zz, h) in enumerate(((zp, 0), (zm, 0), (zp, 1), (zm, 1))):
            out.append(remote(own_src(h, g), panel(g, f), zs.at[g, i], zr.at[g, f], dev(zz, h, x, y)))
        out.append(remote(own_src(nc, g), panel(g, f), zs.at[g, 4], zr.at[g, f], me_partner))
        return out

    def own_local(g):
        return pltpu.make_async_copy(own_src(c, g), panel(g, f), l_sem.at[g])

    def z_wait(g, k):
        remote(panel(g, k), panel(g, k), zs.at[g, 0], zr.at[g, k], me_partner).wait_recv()

    def z_forwards(g):
        return (
            remote(panel(g, 2 * zm), panel(g, 2 * zm), zs.at[g, 5], zr.at[g, 2 * zm], dev(zp, c, x, y)),
            remote(panel(g, 2 * zp + 1), panel(g, 2 * zp + 1), zs.at[g, 6], zr.at[g, 2 * zp + 1], dev(zm, c, x, y)),
        )

    def col_at(cc, yy, g):
        return ((cc * 4 + yy) * CHUNKS + g) * 4

    def x_copies(g):
        out = []
        for i, d in enumerate((2, 1, 3)):
            to = (x + d) % 4
            out.append(remote(f_v.at[g, to], cols.at[col_at(c, y, g) + x], xs.at[g, i], xr.at[g, i], dev(z, c, to, y)))
        return out

    def block(at, size):
        return cols.at[pl.ds(at, size)]

    def to_partner(g, i, yy):
        blk = block(col_at(c, yy, g), 4)
        return remote(blk, blk, ps.at[g, i], pr.at[g, i], me_partner)

    def y_copies(g):
        blk = block(col_at(c, y, g), 4)
        return (
            remote(blk, blk, ys.at[g, 0], yr.at[g, 0], dev(z, c, x, yp)),
            remote(blk, blk, ys.at[g, 1], yr.at[g, 1], dev(z, c, x, ym)),
        )

    def y_forward(g, way):
        if way == 0:
            blk = block(col_at(c, ym, g), 2)
            return remote(blk, blk, ys.at[g, 2], yr.at[g, 2], dev(z, c, x, yp))
        blk = block(col_at(c, yp, g) + 2, 2)
        return remote(blk, blk, ys.at[g, 3], yr.at[g, 3], dev(z, c, x, ym))

    def y_wait(g, i):
        blk = block(col_at(c, y, g), 4 if i < 2 else 2)
        remote(blk, blk, ys.at[g, 0], yr.at[g, i], me_partner).wait_recv()

    def ints_copies():
        return [
            remote(ints, ints_v.at[x], i_sem.at[0, i], i_sem.at[1, i], dev(z, c, (x + d) % 4, y))
            for i, d in enumerate((1, 2, 3))
        ]

    def ens_copies_x():
        return [
            remote(ens, ens_v.at[y, x], e_sem.at[0, i], e_sem.at[1, i], dev(z, c, (x + d) % 4, y))
            for i, d in enumerate((1, 2, 3))
        ]

    def ens_copies_y():
        return [
            remote(ens_v.at[y], ens_v.at[y], e_sem.at[0, 3 + i], e_sem.at[1, 3 + i], dev(z, c, x, (y + d) % 4))
            for i, d in enumerate((1, 2, 3))
        ]

    a_rows = a_v.at[pl.ds(pl.multiple_of(c * PANEL, PANEL), PANEL), :]
    a_partner = remote(fac, a_rows, a_sem.at[0], a_sem.at[1], me_partner)
    a_local = pltpu.make_async_copy(fac, a_rows, a_sem.at[2])
    ints_local = pltpu.make_async_copy(ints, ints_v.at[x], i_sem.at[2, 0])
    ens_local = pltpu.make_async_copy(ens, ens_v.at[y, x], e_sem.at[0, 6])

    def start_own(g):
        for cp in own_copies(g):
            cp.start()
        own_local(g).start()

    start_own(0)
    a_partner.start()
    a_local.start()
    start_own(1)
    for cp in ints_copies() + ens_copies_x():
        cp.start()
    ints_local.start()
    ens_local.start()

    def step(t, carry):
        @pl.when(t < CHUNKS)
        def _():
            z_wait(t, 2 * zm)
            fwd = z_forwards(t)
            fwd[0].start()
            z_wait(t, 2 * zp + 1)
            fwd[1].start()

        @pl.when(t < CHUNKS - 2)
        def _():
            start_own(t + 2)

        @pl.when((t >= 2) & (t < CHUNKS + 2))
        def _():
            g = t - 2
            y_wait(g, 0)
            y_forward(g, 0).start()
            y_wait(g, 1)
            y_forward(g, 1).start()
            to_partner(g, 1, ym).start()
            to_partner(g, 2, yp).start()

        @pl.when(t >= 3)
        def _():
            g = t - 3
            y_wait(g, 2)
            y_wait(g, 3)
            to_partner(g, 3, yo).start()

        @pl.when((t >= 1) & (t < CHUNKS + 1))
        def _():
            g = t - 1

            @pl.when(g == 0)
            def _():
                a_partner.wait_recv()
                a_local.wait()

            own_local(g).wait()
            z_wait(g, 2 * z + nc)
            z_wait(g, 2 * zm + 1)
            z_wait(g, 2 * zp)
            z_wait(g, 2 * zo)
            z_wait(g, 2 * zo + 1)

            def fit(q, carry):
                rows = pl.ds(pl.multiple_of(q * QROWS, QROWS), QROWS)
                acc = jnp.dot(a_v[rows, :], b_v[g], preferred_element_type=F32)
                f_v[g, q] = acc.T.astype(BF16)
                return carry

            lax.fori_loop(0, 4, fit, 0)
            cols[col_at(c, y, g) + x] = f_v[g, x]
            for cp in x_copies(g):
                cp.start()
            for cp in x_copies(g):
                cp.wait_recv()
            for cp in y_copies(g):
                cp.start()
            to_partner(g, 0, y).start()

        return carry

    lax.fori_loop(0, CHUNKS + 3, step, 0)

    for cp in ints_copies() + ens_copies_x():
        cp.wait()
    ints_local.wait()
    ens_local.wait()
    for cp in ens_copies_y():
        cp.start()
    ints_smem = pltpu.make_async_copy(ints_v, ints_s, i_sem.at[2, 1])
    ints_smem.start()
    ints_smem.wait()

    def drain(g, carry):
        for i, yy in enumerate((y, ym, yp, yo)):
            to_partner(g, i, yy).wait()
        for cp in own_copies(g):
            cp.wait_send()
        for cp in z_forwards(g):
            cp.wait_send()
        for cp in x_copies(g):
            cp.wait_send()
        for cp in y_copies(g):
            cp.wait_send()
        for way in (0, 1):
            y_forward(g, way).wait_send()
        return carry

    lax.fori_loop(0, CHUNKS, drain, 0)
    a_partner.wait_send()

    def orbital(xo, position):
        k = ints_s[xo, 1, position]
        t = ints_s[xo, 0, k]
        s = k // 8
        return ((t // 8) * 4 + s % 4) * (CHUNKS * 4) + (t % 8) * 4 + s // 4

    def pairs(half, first):
        def one(i, carry):
            second, slot = i // 4, i % 4
            xo, zo_ = (first, second) if half == 0 else (second, first)
            n = (2 * zo_ + c) * 8 + half * 4 + slot
            left = cols[orbital(xo, 2 * n)]
            right = cols[orbital(xo, 2 * n + 1)]
            e = lax.dot_general(left, right, (((1,), (1,)), ((), ())), preferred_element_type=F32)
            part[half, first, i] = (e * SCALE).astype(BF16)
            return carry

        lax.fori_loop(0, 16, one, 0, unroll=4)

    def rs1_copy(half, d):
        me_at = x if half == 0 else z
        there = (me_at + d) % 4
        to = dev(z, c, there, y) if half == 0 else dev(there, c, x, y)
        return remote(part.at[half, there], rs1.at[half, d - 1], r_sem.at[0, half, d], r_sem.at[1, half, d], to)

    def rs2_copy(half, d):
        me_at = z if half == 0 else x
        there = (me_at + d) % 4
        to = dev(there, c, x, y) if half == 0 else dev(z, c, there, y)
        return remote(summed.at[half, pl.ds(there * 4, 4)], rs2.at[half, d - 1], r_sem.at[2, half, d], r_sem.at[3, half, d], to)

    for d in (2, 1, 3, 0):
        pairs(0, (x + d) % 4)
        pairs(1, (z + d) % 4)
        if d:
            rs1_copy(0, d).start()
            rs1_copy(1, d).start()

    for cp in ens_copies_y():
        cp.wait()
    ens_smem = pltpu.make_async_copy(ens_v, ens_s, e_sem.at[1, 6])
    ens_smem.start()
    ens_smem.wait()
    live = ints_s[x, 2, 0]

    def energy(position):
        k = ints_s[x, 1, position]
        t = ints_s[x, 0, k]
        s = k // 8
        return ens_s[s % 4, s // 4, 0, t]

    for slot in range(8):
        n = f * 8 + slot
        denom = cabs[...] - (energy(2 * n) + energy(2 * n + 1))
        rec_out[pl.ds(slot, 1), :] = jnp.where(n < live, 1.0 / denom, 0.0)

    for half in (0, 1):
        me_at = x if half == 0 else z
        for d in (1, 2, 3):
            rs1_copy(half, d).wait_recv()

        def add(i, carry):
            total = part[half, me_at, i].astype(F32)
            for d in (0, 1, 2):
                total = total + rs1[half, d, i].astype(F32)
            summed[half, i] = total.astype(BF16)
            return carry

        lax.fori_loop(0, 16, add, 0)
        for d in (2, 1, 3):
            rs2_copy(half, d).start()

    for half in (0, 1):
        me_at = z if half == 0 else x
        for d in (1, 2, 3):
            rs2_copy(half, d).wait_recv()

        for i in range(4):
            total = summed[half, me_at * 4 + i].astype(F32)
            for d in (0, 1, 2):
                total = total + rs2[half, d, i].astype(F32)
            exch_out[half * 4 + i] = total.astype(BF16)

    for half in (0, 1):
        for d in (1, 2, 3):
            rs1_copy(half, d).wait_send()
            rs2_copy(half, d).wait_send()


def project_kernel(exch, coupling, rec, out):
    weighted = jnp.dot(exch[0], coupling[...], preferred_element_type=F32)
    out[0] = (weighted * rec[0]).astype(BF16)


def on_device(fac, tri, send_map, pair_slots, pair_count, orbital_energy, cabs_energy, coupling):
    dma = pltpu.SemaphoreType.DMA
    ints = jnp.concatenate(
        [
            send_map.reshape(1, LANES),
            pair_slots,
            jnp.broadcast_to(pair_count[:, None], (6, LANES)),
        ],
        axis=0,
    )
    ens = jnp.broadcast_to(jnp.pad(orbital_energy.astype(F32), (0, LANES - 16))[None, :], (8, LANES))
    hbm = pl.BlockSpec(memory_space=pl.ANY)
    vmem = pl.BlockSpec(memory_space=pltpu.VMEM)
    exch, rec = pl.pallas_call(
        fused_kernel,
        out_shape=(
            jax.ShapeDtypeStruct((8, LANES, LANES), BF16),
            jax.ShapeDtypeStruct((8, 1024), F32),
        ),
        in_specs=[hbm, hbm, hbm, hbm, vmem],
        out_specs=(vmem, vmem),
        scratch_shapes=[
            pltpu.VMEM((2 * PANEL, 4096), BF16),
            pltpu.VMEM((CHUNKS, 4096, LANES), BF16),
            pltpu.VMEM((CHUNKS, 4, LANES, QROWS), BF16),
            pltpu.VMEM((256, LANES, QROWS), BF16),
            pltpu.VMEM((2, 4, 16, LANES, LANES), BF16),
            pltpu.VMEM((2, 3, 16, LANES, LANES), BF16),
            pltpu.VMEM((2, 16, LANES, LANES), BF16),
            pltpu.VMEM((2, 3, 4, LANES, LANES), BF16),
            pltpu.VMEM((4, 8, LANES), jnp.int32),
            pltpu.VMEM((4, 4, 8, LANES), F32),
            pltpu.SMEM((4, 8, LANES), jnp.int32),
            pltpu.SMEM((4, 4, 8, LANES), F32),
            dma((3,)),
            dma((CHUNKS, 7)),
            dma((CHUNKS, 8)),
            dma((CHUNKS, 3)),
            dma((CHUNKS, 3)),
            dma((CHUNKS, 4)),
            dma((CHUNKS, 4)),
            dma((CHUNKS, 4)),
            dma((CHUNKS, 4)),
            dma((3, 3)),
            dma((2, 7)),
            dma((4, 2, 4)),
            dma((CHUNKS,)),
        ],
        compiler_params=pltpu.CompilerParams(
            collective_id=0, has_side_effects=True, vmem_limit_bytes=64 * 1024 * 1024 - 65536
        ),
        name="fit_exchange",
    )(fac, tri, ints, ens, cabs_energy.reshape(1, 1024))
    projected = pl.pallas_call(
        project_kernel,
        grid=(8,),
        out_shape=jax.ShapeDtypeStruct((8, LANES, 1024), BF16),
        in_specs=[
            pl.BlockSpec((1, LANES, LANES), lambda i: (i, 0, 0)),
            pl.BlockSpec((LANES, 1024), lambda i: (0, 0)),
            pl.BlockSpec((1, 1, 1024), lambda i: (i, 0, 0)),
        ],
        out_specs=pl.BlockSpec((1, LANES, 1024), lambda i: (i, 0, 0)),
        name="project",
    )(exch, coupling, rec.reshape(8, 1, 1024))
    return projected.reshape(1, 8, LANES, 1024)


def solution(mesh):
    in_specs = (
        P("fit", None),
        P("fit", "pair"),
        P("pair", None, None),
        P("pair", None),
        P("pair"),
        P("pair"),
        P(),
        P(),
    )
    return jax.shard_map(
        on_device, mesh=mesh, in_specs=in_specs, out_specs=P("pair", "fit", None, None), check_vma=False
    )
```

```python
import jax
import jax.numpy as jnp
from jax import lax
from jax.experimental import pallas as pl
from jax.experimental.pallas import tpu as pltpu
from jax.sharding import PartitionSpec as P

MESH = pl.DeviceIdType.MESH
F32 = jnp.float32
BF16 = jnp.bfloat16
CHUNKS = 8
LANES = 128
PANEL = 512
QROWS = 256
SCALE = 4096.0 ** -0.5


def fused_kernel(
    fac, tri, wanted, slots, ens, cabs, count,
    exch_out, rec_out,
    a_v, b_v, f_v, cols, part, rs_far, rs_near, summed, rs2,
    wanted_v, slots_v, ens_v, wanted_s, slots_s, ens_s,
    a_sem, zs, zr, xs, xr, ys, yr, ps, pr, i_sem, e_sem, r_sem, l_sem,
):
    f = lax.axis_index("fit")
    p = lax.axis_index("pair")
    z, c = f // 2, f % 2
    x, y = p // 4, p % 4
    nc = 1 - c
    zp, zm, zo = (z + 1) % 4, (z + 3) % 4, (z + 2) % 4
    yp, ym, yo = (y + 1) % 4, (y + 3) % 4, (y + 2) % 4

    def dev(zz, cc, xx, yy):
        return (2 * zz + cc, 4 * xx + yy)

    me_partner = dev(z, nc, x, y)

    def remote(src, dst, ss, rs, to):
        return pltpu.make_async_remote_copy(
            src_ref=src, dst_ref=dst, send_sem=ss, recv_sem=rs, device_id=to, device_id_type=MESH
        )

    barrier = pltpu.get_barrier_semaphore()
    greeted = [me_partner]
    for d in (1, 2, 3):
        greeted.append(dev((z + d) % 4, c, x, y))
        greeted.append(dev(z, c, (x + d) % 4, y))
        greeted.append(dev(z, c, x, (y + d) % 4))
    greeted.append(dev(zp, nc, x, y))
    greeted.append(dev(zm, nc, x, y))
    for to in greeted:
        pl.semaphore_signal(barrier, inc=1, device_id=to, device_id_type=MESH)
    pl.semaphore_wait(barrier, len(greeted))

    def own_src(h, g):
        return tri.at[:, pl.ds(pl.multiple_of((h * CHUNKS + g) * LANES, LANES), LANES)]

    def panel(g, k):
        return b_v.at[g, pl.ds(pl.multiple_of(k * PANEL, PANEL), PANEL), :]

    def own_copies(g):
        out = []
        for i, (zz, h) in enumerate(((zp, 0), (zm, 0), (zp, 1), (zm, 1))):
            out.append(remote(own_src(h, g), panel(g, f), zs.at[g, i], zr.at[g, f], dev(zz, h, x, y)))
        out.append(remote(own_src(nc, g), panel(g, f), zs.at[g, 4], zr.at[g, f], me_partner))
        return out

    def own_local(g):
        return pltpu.make_async_copy(own_src(c, g), panel(g, f), l_sem.at[g])

    def z_wait(g, k):
        remote(panel(g, k), panel(g, k), zs.at[g, 0], zr.at[g, k], me_partner).wait_recv()

    def z_forwards(g):
        return (
            remote(panel(g, 2 * zm), panel(g, 2 * zm), zs.at[g, 5], zr.at[g, 2 * zm], dev(zp, c, x, y)),
            remote(panel(g, 2 * zp + 1), panel(g, 2 * zp + 1), zs.at[g, 6], zr.at[g, 2 * zp + 1], dev(zm, c, x, y)),
        )

    def col_at(cc, yy, g):
        return ((cc * 4 + yy) * CHUNKS + g) * 4

    def x_copy(g, i):
        to = (x + 3 - i) % 4
        return remote(f_v.at[g, to], cols.at[col_at(c, y, g) + x], xs.at[g, i], xr.at[g, i], dev(z, c, to, y))

    def x_wait(g, i):
        at = cols.at[col_at(c, y, g)]
        remote(at, at, xs.at[g, 0], xr.at[g, i], me_partner).wait_recv()

    def block(at, size):
        return cols.at[pl.ds(at, size)]

    def to_partner(g, i, yy):
        blk = block(col_at(c, yy, g), 4)
        return remote(blk, blk, ps.at[g, i], pr.at[g, i], me_partner)

    def y_copies(g):
        blk = block(col_at(c, y, g), 4)
        return (
            remote(blk, blk, ys.at[g, 0], yr.at[g, 0], dev(z, c, x, yp)),
            remote(blk, blk, ys.at[g, 1], yr.at[g, 1], dev(z, c, x, ym)),
        )

    def y_forward(g, way):
        if way == 0:
            blk = block(col_at(c, ym, g), 2)
            return remote(blk, blk, ys.at[g, 2], yr.at[g, 2], dev(z, c, x, yp))
        blk = block(col_at(c, yp, g) + 2, 2)
        return remote(blk, blk, ys.at[g, 3], yr.at[g, 3], dev(z, c, x, ym))

    def y_wait(g, i):
        blk = block(col_at(c, y, g), 4 if i < 2 else 2)
        remote(blk, blk, ys.at[g, 0], yr.at[g, i], me_partner).wait_recv()

    def ints_copies():
        out = []
        for i, d in enumerate((1, 2, 3)):
            to = dev(z, c, (x + d) % 4, y)
            out.append(remote(wanted.at[0], wanted_v.at[x], i_sem.at[0, i], i_sem.at[1, i], to))
            out.append(remote(slots, slots_v.at[x], i_sem.at[2, i], i_sem.at[3, i], to))
        return out

    def ens_copies_x():
        return [
            remote(ens, ens_v.at[y, x], e_sem.at[0, i], e_sem.at[1, i], dev(z, c, (x + d) % 4, y))
            for i, d in enumerate((1, 2, 3))
        ]

    def ens_copies_y():
        return [
            remote(ens_v.at[y], ens_v.at[y], e_sem.at[0, 3 + i], e_sem.at[1, 3 + i], dev(z, c, x, (y + d) % 4))
            for i, d in enumerate((1, 2, 3))
        ]

    a_rows = a_v.at[pl.ds(pl.multiple_of(c * PANEL, PANEL), PANEL), :]
    a_partner = remote(fac, a_rows, a_sem.at[0], a_sem.at[1], me_partner)
    a_local = pltpu.make_async_copy(fac, a_rows, a_sem.at[2])
    small_local = (
        pltpu.make_async_copy(wanted.at[0], wanted_v.at[x], i_sem.at[0, 3]),
        pltpu.make_async_copy(slots, slots_v.at[x], i_sem.at[1, 3]),
        pltpu.make_async_copy(ens, ens_v.at[y, x], e_sem.at[0, 6]),
    )

    def start_own(g):
        for cp in own_copies(g):
            cp.start()
        own_local(g).start()

    start_own(0)
    a_partner.start()
    a_local.start()
    for cp in ints_copies() + ens_copies_x():
        cp.start()
    for cp in small_local:
        cp.start()

    def step(t, carry):
        @pl.when(t < CHUNKS)
        def _():
            z_wait(t, 2 * zm)
            fwd = z_forwards(t)
            fwd[0].start()
            z_wait(t, 2 * zp + 1)
            fwd[1].start()

        @pl.when(t == 0)
        def _():
            start_own(1)

        @pl.when(t < CHUNKS - 2)
        def _():
            start_own(t + 2)

        @pl.when((t == 1) | ((t >= 3) & (t < CHUNKS + 2)))
        def _():
            g = jnp.maximum(t - 2, 0)
            for i in range(3):
                x_wait(g, i)
            for cp in y_copies(g):
                cp.start()
            to_partner(g, 0, y).start()

        @pl.when((t == 0) | ((t >= 2) & (t < CHUNKS + 1)))
        def _():
            g = jnp.maximum(t - 1, 0)

            @pl.when(g == 0)
            def _():
                a_partner.wait_recv()
                a_local.wait()

            own_local(g).wait()
            z_wait(g, 2 * z + nc)
            z_wait(g, 2 * zm + 1)
            z_wait(g, 2 * zp)
            z_wait(g, 2 * zo)
            z_wait(g, 2 * zo + 1)

            def fit(q):
                rows = pl.ds(pl.multiple_of(q * QROWS, QROWS), QROWS)
                acc = jnp.dot(a_v[rows, :], b_v[g], preferred_element_type=F32)
                return acc.T.astype(BF16)

            def fit_send(i, carry):
                q = (x + 3 - i) % 4
                f_v[g, q] = fit(q)
                x_copy(g, i).start()
                return carry

            lax.fori_loop(0, 3, fit_send, 0)
            cols[col_at(c, y, g) + x] = fit(x)

        @pl.when((t >= 3) & (t < CHUNKS + 3))
        def _():
            g = t - 3
            y_wait(g, 0)
            y_forward(g, 0).start()
            y_wait(g, 1)
            y_forward(g, 1).start()
            to_partner(g, 1, ym).start()
            to_partner(g, 2, yp).start()

        @pl.when(t >= 4)
        def _():
            g = t - 4
            y_wait(g, 2)
            y_wait(g, 3)
            to_partner(g, 3, yo).start()

        @pl.when(t == 2)
        def _():
            for cp in ints_copies() + ens_copies_x():
                cp.wait()
            for cp in small_local:
                cp.wait()
            for cp in ens_copies_y():
                cp.start()

        @pl.when(t == 6)
        def _():
            for cp in ens_copies_y():
                cp.wait()
            to_smem = (
                pltpu.make_async_copy(wanted_v, wanted_s, i_sem.at[2, 3]),
                pltpu.make_async_copy(slots_v, slots_s, i_sem.at[3, 3]),
                pltpu.make_async_copy(ens_v, ens_s, e_sem.at[1, 6]),
            )
            for cp in to_smem:
                cp.start()
            for cp in to_smem:
                cp.wait()

        return carry

    lax.fori_loop(0, CHUNKS + 4, step, 0)

    def drain(g, carry):
        for i, yy in enumerate((y, ym, yp, yo)):
            to_partner(g, i, yy).wait()
        for cp in own_copies(g):
            cp.wait_send()
        for cp in z_forwards(g):
            cp.wait_send()
        for i in range(3):
            x_copy(g, i).wait_send()
        for cp in y_copies(g):
            cp.wait_send()
        for way in (0, 1):
            y_forward(g, way).wait_send()
        return carry

    lax.fori_loop(0, CHUNKS, drain, 0)
    a_partner.wait_send()

    def orbital(xo, position):
        k = slots_s[xo, 0, position]
        s = k >> 3
        t = wanted_s[xo, s, k & 7]
        return ((t >> 3) << 7) + ((s & 3) << 5) + ((t & 7) << 2) + (s >> 2)

    def pairs(half, first):
        def some(j, carry):
            done = []
            for slot in range(8):
                second = 2 * j + slot // 4
                xo, zz = (first, second) if half == 0 else (second, first)
                n = (2 * zz + c) * 8 + half * 4 + slot % 4
                left = cols[orbital(xo, 2 * n)]
                right = cols[orbital(xo, 2 * n + 1)]
                e = lax.dot_general(left, right, (((1,), (1,)), ((), ())), preferred_element_type=F32)
                done.append((e * SCALE).astype(BF16))
            for slot in range(8):
                part[half, first, j * 8 + slot] = done[slot]
            return carry

        lax.fori_loop(0, 2, some, 0)

    def ring(half, d):
        if half == 0:
            at = (x + d) % 4
            return at, dev(z, c, at, y)
        at = (z + d) % 4
        return at, dev(at, c, x, y)

    def far_copy(half, i):
        far, _ = ring(half, 2)
        _, to = ring(half, 3 if i == 0 else 1)
        return remote(part.at[half, far, pl.ds(8 * i, 8)], rs_far.at[half, i], r_sem.at[0, half, i], r_sem.at[1, half, i], to)

    def near_copy(half, i, summed_part):
        at, to = ring(half, 3 if i == 0 else 1)
        first = 8 * i if summed_part else 8 - 8 * i
        j = 2 * i + (1 if summed_part else 0)
        rows = pl.ds(first, 8)
        return remote(part.at[half, at, rows], rs_near.at[half, i, rows], r_sem.at[2, half, j], r_sem.at[3, half, j], to)

    def combine(half, i):
        at, _ = ring(half, 3 if i == 0 else 1)
        far_copy(half, i).wait_recv()

        def add(k, carry):
            part[half, at, 8 * i + k] = (part[half, at, 8 * i + k].astype(F32) + rs_far[half, i, k].astype(F32)).astype(BF16)
            return carry

        lax.fori_loop(0, 8, add, 0, unroll=2)

    def rs2_copy(half, d):
        there, to = ring(1 - half, d)
        return remote(summed.at[half, pl.ds(there * 4, 4)], rs2.at[half, d - 1], r_sem.at[4, half, d], r_sem.at[5, half, d], to)

    pairs(0, ring(0, 2)[0])
    pairs(1, ring(1, 2)[0])
    for i in (0, 1):
        far_copy(0, i).start()
        far_copy(1, i).start()
    for i, d in ((0, 3), (1, 1)):
        pairs(0, ring(0, d)[0])
        pairs(1, ring(1, d)[0])
        near_copy(0, i, False).start()
        near_copy(1, i, False).start()
    pairs(0, x)
    pairs(1, z)
    for half in (0, 1):
        for i in (0, 1):
            combine(half, i)
            near_copy(half, i, True).start()

    live = count[0]

    def energy(position):
        k = slots_s[x, 0, position]
        s = k >> 3
        return ens_s[s & 3, s >> 2, 0, wanted_s[x, s, k & 7]]

    for slot in range(8):
        n = f * 8 + slot
        denom = cabs[...] - (energy(2 * n) + energy(2 * n + 1))
        rec_out[slot] = jnp.where(n < live, 1.0 / denom, 0.0)

    for half in (0, 1):
        me_at = x if half == 0 else z
        for i in (0, 1):
            near_copy(half, i, False).wait_recv()
            near_copy(half, i, True).wait_recv()

        def add(i, carry):
            total = part[half, me_at, i].astype(F32)
            for d in (0, 1):
                total = total + rs_near[half, d, i].astype(F32)
            summed[half, i] = total.astype(BF16)
            return carry

        lax.fori_loop(0, 16, add, 0, unroll=2)
        for d in (2, 1, 3):
            rs2_copy(half, d).start()

    for half in (0, 1):
        me_at = z if half == 0 else x
        for d in (1, 2, 3):
            rs2_copy(half, d).wait_recv()

        for i in range(4):
            total = summed[half, me_at * 4 + i].astype(F32)
            for d in (0, 1, 2):
                total = total + rs2[half, d, i].astype(F32)
            exch_out[half * 4 + i] = total.astype(BF16)

    for half in (0, 1):
        for i in (0, 1):
            far_copy(half, i).wait_send()
            near_copy(half, i, False).wait_send()
            near_copy(half, i, True).wait_send()
        for d in (1, 2, 3):
            rs2_copy(half, d).wait_send()


def project_kernel(exch, coupling, rec, out):
    weighted = jnp.dot(exch[0], coupling[...], preferred_element_type=F32)
    out[0] = (weighted * rec[0]).astype(BF16)


def on_device(fac, tri, send_map, pair_slots, pair_count, orbital_energy, cabs_energy, coupling):
    dma = pltpu.SemaphoreType.DMA
    ens = jnp.broadcast_to(orbital_energy.astype(F32)[None, :], (8, 16))
    hbm = pl.BlockSpec(memory_space=pl.ANY)
    vmem = pl.BlockSpec(memory_space=pltpu.VMEM)
    exch, rec = pl.pallas_call(
        fused_kernel,
        out_shape=(
            jax.ShapeDtypeStruct((8, LANES, LANES), BF16),
            jax.ShapeDtypeStruct((8, 1, 1024), F32),
        ),
        in_specs=[hbm, hbm, hbm, hbm, hbm, vmem, pl.BlockSpec(memory_space=pltpu.SMEM)],
        out_specs=(vmem, vmem),
        scratch_shapes=[
            pltpu.VMEM((2 * PANEL, 4096), BF16),
            pltpu.VMEM((CHUNKS, 4096, LANES), BF16),
            pltpu.VMEM((CHUNKS, 4, LANES, QROWS), BF16),
            pltpu.VMEM((256, LANES, QROWS), BF16),
            pltpu.VMEM((2, 4, 16, LANES, LANES), BF16),
            pltpu.VMEM((2, 2, 8, LANES, LANES), BF16),
            pltpu.VMEM((2, 2, 16, LANES, LANES), BF16),
            pltpu.VMEM((2, 16, LANES, LANES), BF16),
            pltpu.VMEM((2, 3, 4, LANES, LANES), BF16),
            pltpu.VMEM((4, 16, 8), jnp.int32),
            pltpu.VMEM((4, 1, LANES), jnp.int32),
            pltpu.VMEM((4, 4, 8, 16), F32),
            pltpu.SMEM((4, 16, 8), jnp.int32),
            pltpu.SMEM((4, 1, LANES), jnp.int32),
            pltpu.SMEM((4, 4, 8, 16), F32),
            dma((3,)),
            dma((CHUNKS, 7)),
            dma((CHUNKS, 8)),
            dma((CHUNKS, 3)),
            dma((CHUNKS, 3)),
            dma((CHUNKS, 4)),
            dma((CHUNKS, 4)),
            dma((CHUNKS, 4)),
            dma((CHUNKS, 4)),
            dma((4, 4)),
            dma((2, 7)),
            dma((6, 2, 4)),
            dma((CHUNKS,)),
        ],
        compiler_params=pltpu.CompilerParams(
            collective_id=0, has_side_effects=True, vmem_limit_bytes=64 * 1024 * 1024 - 65536
        ),
        name="fit_exchange",
    )(fac, tri, send_map, pair_slots, ens, cabs_energy.reshape(1, 1024), pair_count)
    projected = pl.pallas_call(
        project_kernel,
        grid=(8,),
        out_shape=jax.ShapeDtypeStruct((8, LANES, 1024), BF16),
        in_specs=[
            pl.BlockSpec((1, LANES, LANES), lambda i: (i, 0, 0)),
            pl.BlockSpec((LANES, 1024), lambda i: (0, 0)),
            pl.BlockSpec((1, 1, 1024), lambda i: (i, 0, 0)),
        ],
        out_specs=pl.BlockSpec((1, LANES, 1024), lambda i: (i, 0, 0)),
        name="project",
    )(exch, coupling, rec)
    return projected.reshape(1, 8, LANES, 1024)


def solution(mesh):
    in_specs = (
        P("fit", None),
        P("fit", "pair"),
        P("pair", None, None),
        P("pair", None),
        P("pair"),
        P("pair"),
        P(),
        P(),
    )
    return jax.shard_map(
        on_device, mesh=mesh, in_specs=in_specs, out_specs=P("pair", "fit", None, None), check_vma=False
    )
```

```python
import jax
import jax.numpy as jnp
from jax import lax
from jax.experimental import pallas as pl
from jax.experimental.pallas import tpu as pltpu
from jax.sharding import PartitionSpec as P

MESH = pl.DeviceIdType.MESH
F32 = jnp.float32
BF16 = jnp.bfloat16
CHUNKS = 8
LANES = 128
PANEL = 512
QROWS = 256
SCALE = 4096.0 ** -0.5


def fused_kernel(
    fac, tri, wanted, slots, ens, cabs, coupling, count,
    out,
    a_v, b_v, f_v, cols, part, rs_far, rs_near, summed, rs2,
    wanted_v, slots_v, ens_v, wanted_s, slots_s, ens_s, rec_v, out_v,
    send_sem, a_sem, zr, xr, yr, pr, i_sem, e_sem, r_sem, l_sem, o_sem,
):
    f = lax.axis_index("fit")
    p = lax.axis_index("pair")
    z, c = f // 2, f % 2
    x, y = p // 4, p % 4
    nc = 1 - c
    zp, zm, zo = (z + 1) % 4, (z + 3) % 4, (z + 2) % 4
    yp, ym, yo = (y + 1) % 4, (y + 3) % 4, (y + 2) % 4

    def dev(zz, cc, xx, yy):
        return (2 * zz + cc, 4 * xx + yy)

    me_partner = dev(z, nc, x, y)

    def remote(src, dst, ss, rs, to):
        return pltpu.make_async_remote_copy(
            src_ref=src, dst_ref=dst, send_sem=ss, recv_sem=rs, device_id=to, device_id_type=MESH
        )

    barrier = pltpu.get_barrier_semaphore()
    greeted = [me_partner]
    for d in (1, 2, 3):
        greeted.append(dev((z + d) % 4, c, x, y))
        greeted.append(dev(z, c, (x + d) % 4, y))
        greeted.append(dev(z, c, x, (y + d) % 4))
    greeted.append(dev(zp, nc, x, y))
    greeted.append(dev(zm, nc, x, y))
    for to in greeted:
        pl.semaphore_signal(barrier, inc=1, device_id=to, device_id_type=MESH)

    def own_src(h, g):
        return tri.at[:, pl.ds(pl.multiple_of((h * CHUNKS + g) * LANES, LANES), LANES)]

    def panel(g, k):
        return b_v.at[g, pl.ds(pl.multiple_of(k * PANEL, PANEL), PANEL), :]

    def own_first(g):
        return (
            remote(own_src(c, g), panel(g, f), send_sem.at[0], zr.at[g, 0], dev(zp, c, x, y)),
            remote(own_src(c, g), panel(g, f), send_sem.at[0], zr.at[g, 2], dev(zm, c, x, y)),
        )

    def own_second(g):
        return (
            remote(own_src(nc, g), panel(g, f), send_sem.at[0], zr.at[g, 2], dev(zp, nc, x, y)),
            remote(own_src(nc, g), panel(g, f), send_sem.at[0], zr.at[g, 1], dev(zm, nc, x, y)),
            remote(own_src(nc, g), panel(g, f), send_sem.at[0], zr.at[g, 2], me_partner),
        )

    def start(copies):
        for cp in copies:
            cp.start()

    def own_local(g):
        return pltpu.make_async_copy(own_src(c, g), panel(g, f), l_sem)

    def z_forward(g, way):
        k = 2 * zm + c if way == 0 else 2 * zp + nc
        return remote(panel(g, k), panel(g, k), send_sem.at[0], zr.at[g, 2], dev(zp if way == 0 else zm, c, x, y))

    def z_wait(g, i):
        blk = b_v.at[g, pl.ds(0, PANEL if i < 2 else 5 * PANEL), :]
        remote(blk, blk, send_sem.at[0], zr.at[g, i], me_partner).wait_recv()

    def col_at(cc, yy, g):
        return ((cc * 4 + yy) * CHUNKS + g) * 4

    def x_copy(g, i):
        to = (x + 3 - i) % 4
        return remote(f_v.at[g, to], cols.at[col_at(c, y, g) + x], send_sem.at[1], xr.at[g, i], dev(z, c, to, y))

    def x_wait(g, i):
        at = cols.at[col_at(c, y, g)]
        remote(at, at, send_sem.at[1], xr.at[g, i], me_partner).wait_recv()

    def block(at, size):
        return cols.at[pl.ds(at, size)]

    def to_partner(g, yy):
        blk = block(col_at(c, yy, g), 4)
        return remote(blk, blk, send_sem.at[3], pr, me_partner)

    def y_copy(g, way, i):
        blk = cols.at[col_at(c, y, g) + (x + 1 + i) % 4]
        j = ((4, 1, 4, 0), (2, 5, 3, 5))[way][i]
        return remote(blk, blk, send_sem.at[2], yr.at[g, j], dev(z, c, x, yp if way == 0 else ym))

    def y_start(g, i):
        y_copy(g, 0, i).start()
        y_copy(g, 1, i).start()

    def y_forward(g, i):
        yy, to = (ym, yp) if i % 2 else (yp, ym)
        blk = cols.at[col_at(c, yy, g) + (x + 1 + i) % 4]
        return remote(blk, blk, send_sem.at[2], yr.at[g, 6], dev(z, c, x, to))

    def y_wait(g, j):
        blk = block(col_at(c, y, g), (1, 1, 1, 1, 2, 2, 4)[j])
        remote(blk, blk, send_sem.at[2], yr.at[g, j], me_partner).wait_recv()

    def ints_copies():
        out = []
        for i, d in enumerate((1, 2, 3)):
            to = dev(z, c, (x + d) % 4, y)
            out.append(remote(wanted.at[0], wanted_v.at[x], i_sem.at[0, i], i_sem.at[1, i], to))
            out.append(remote(slots, slots_v.at[x], i_sem.at[2, i], i_sem.at[3, i], to))
        return out

    def ens_copies_x():
        return [
            remote(ens, ens_v.at[y, x], e_sem.at[0, i], e_sem.at[1, i], dev(z, c, (x + d) % 4, y))
            for i, d in enumerate((1, 2, 3))
        ]

    def ens_copies_y():
        return [
            remote(ens_v.at[y], ens_v.at[y], e_sem.at[0, 3 + i], e_sem.at[1, 3 + i], dev(z, c, x, (y + d) % 4))
            for i, d in enumerate((1, 2, 3))
        ]

    a_rows = a_v.at[pl.ds(pl.multiple_of(c * PANEL, PANEL), PANEL), :]
    a_partner = remote(fac, a_rows, a_sem.at[0], a_sem.at[1], me_partner)
    a_local = pltpu.make_async_copy(fac, a_rows, a_sem.at[2])
    small_local = (
        pltpu.make_async_copy(wanted.at[0], wanted_v.at[x], i_sem.at[0, 3]),
        pltpu.make_async_copy(slots, slots_v.at[x], i_sem.at[1, 3]),
        pltpu.make_async_copy(ens, ens_v.at[y, x], e_sem.at[0, 6]),
    )

    for g in range(CHUNKS):
        own_local(g).start()
    a_local.start()
    for cp in small_local:
        cp.start()

    pl.semaphore_wait(barrier, len(greeted))

    @pl.when(c == 0)
    def _():
        start(own_first(0))
        start(own_second(0))

    @pl.when(c == 1)
    def _():
        start(own_second(0))
        start(own_first(0))

    a_partner.start()
    for cp in ints_copies() + ens_copies_x():
        cp.start()

    def step(t, carry):
        @pl.when(t < CHUNKS)
        def _():
            z_wait(t, 0)
            z_forward(t, 0).start()
            z_wait(t, 1)
            z_forward(t, 1).start()

        @pl.when(c == 0)
        def _():
            @pl.when(t == 0)
            def _():
                start(own_first(1))

            @pl.when(t < CHUNKS - 1)
            def _():
                start(own_second(t + 1))

            @pl.when(t < CHUNKS - 2)
            def _():
                start(own_first(t + 2))

        @pl.when(c == 1)
        def _():
            @pl.when(t == 0)
            def _():
                start(own_second(1))

            @pl.when(t < CHUNKS - 1)
            def _():
                start(own_first(t + 1))

            @pl.when(t < CHUNKS - 2)
            def _():
                start(own_second(t + 2))

        def send_rest(g):
            for i in (0, 2, 1):
                x_wait(g, i)
                y_start(g, i)
            to_partner(g, y).start()

        @pl.when((t == 1) | ((t >= 3) & (t < CHUNKS)))
        def _():
            send_rest(jnp.maximum(t - 2, 0))

        @pl.when((t == 0) | ((t >= 2) & (t < CHUNKS + 1)))
        def _():
            g = jnp.maximum(t - 1, 0)

            @pl.when(t == 0)
            def _():
                a_partner.wait_recv()
                a_local.wait()
                pltpu.make_async_copy(b_v.at[0], b_v.at[0], l_sem).wait()

            z_wait(g, 2)

            def fit(q):
                rows = pl.ds(pl.multiple_of(q * QROWS, QROWS), QROWS)
                acc = jnp.dot(a_v[rows, :], b_v[g], preferred_element_type=F32)
                return acc.T.astype(BF16)

            cols[col_at(c, y, g) + x] = fit(x)

            def fit_send(j, carry):
                i = jnp.where(j < 2, 1 - j, 2)
                q = (x + 3 - i) % 4
                f_v[g, q] = fit(q)
                x_copy(g, i).start()

                @pl.when(j == 0)
                def _():
                    y_start(g, 3)

                return carry

            lax.fori_loop(0, 3, fit_send, 0)

        @pl.when(t == CHUNKS)
        def _():
            send_rest(CHUNKS - 2)

        @pl.when((t >= 3) & (t < CHUNKS + 3))
        def _():
            g = t - 3
            for j, i in ((0, 3), (2, 0), (3, 2), (1, 1)):
                y_wait(g, j)
                y_forward(g, i).start()
            y_wait(g, 4)
            y_wait(g, 5)
            to_partner(g, ym).start()
            to_partner(g, yp).start()

        @pl.when(t == CHUNKS)
        def _():
            send_rest(CHUNKS - 1)

        @pl.when(t >= 4)
        def _():
            y_wait(t - 4, 6)
            to_partner(t - 4, yo).start()

        @pl.when(t == 2)
        def _():
            for cp in ints_copies() + ens_copies_x():
                cp.wait()
            for cp in small_local:
                cp.wait()
            for cp in ens_copies_y():
                cp.start()

        @pl.when(t == 6)
        def _():
            for cp in ens_copies_y():
                cp.wait()
            to_smem = (
                pltpu.make_async_copy(wanted_v, wanted_s, i_sem.at[2, 3]),
                pltpu.make_async_copy(slots_v, slots_s, i_sem.at[3, 3]),
                pltpu.make_async_copy(ens_v, ens_s, e_sem.at[1, 6]),
            )
            for cp in to_smem:
                cp.start()
            for cp in to_smem:
                cp.wait()

        return carry

    lax.fori_loop(0, CHUNKS + 4, step, 0)

    def sent(ref, sem):
        remote(ref, ref, sem, pr, me_partner).wait_send()

    remote(b_v, b_v, send_sem.at[3], pr, me_partner).wait_recv()
    sent(b_v.at[pl.ds(0, 7)], send_sem.at[0])
    sent(f_v.at[pl.ds(0, 6)], send_sem.at[1])
    sent(b_v.at[pl.ds(0, 6)], send_sem.at[2])
    sent(b_v, send_sem.at[3])
    a_partner.wait_send()

    def orbital(xo, position):
        k = slots_s[xo, 0, position]
        s = k >> 3
        t = wanted_s[xo, k & 7, s]
        return ((t >> 3) << 7) + ((s & 3) << 5) + ((t & 7) << 2) + (s >> 2)

    def pairs(half, first):
        def some(j, carry):
            done = []
            for slot in range(8):
                second = 2 * j + slot // 4
                xo, zz = (first, second) if half == 0 else (second, first)
                n = (2 * zz + c) * 8 + half * 4 + slot % 4
                left = cols[orbital(xo, 2 * n)]
                right = cols[orbital(xo, 2 * n + 1)]
                e = lax.dot_general(left, right, (((1,), (1,)), ((), ())), preferred_element_type=F32)
                done.append((e * SCALE).astype(BF16))
            for slot in range(8):
                part[half, first, j * 8 + slot] = done[slot]
            return carry

        lax.fori_loop(0, 2, some, 0)

    def ring(half, d):
        if half == 0:
            at = (x + d) % 4
            return at, dev(z, c, at, y)
        at = (z + d) % 4
        return at, dev(at, c, x, y)

    def far_copy(half, i):
        far, _ = ring(half, 2)
        _, to = ring(half, 3 if i == 0 else 1)
        return remote(part.at[half, far, pl.ds(8 * i, 8)], rs_far.at[half, i], send_sem.at[4], r_sem.at[0, half, i], to)

    def near_copy(half, i, summed_part):
        at, to = ring(half, 3 if i == 0 else 1)
        first = 8 * i if summed_part else 8 - 8 * i
        j = 2 * i + (1 if summed_part else 0)
        rows = pl.ds(first, 8)
        return remote(part.at[half, at, rows], rs_near.at[half, i, rows], send_sem.at[4], r_sem.at[1, half, j], to)

    def combine(half, i):
        at, _ = ring(half, 3 if i == 0 else 1)
        far_copy(half, i).wait_recv()

        def add(k, carry):
            part[half, at, 8 * i + k] = (part[half, at, 8 * i + k].astype(F32) + rs_far[half, i, k].astype(F32)).astype(BF16)
            return carry

        lax.fori_loop(0, 8, add, 0, unroll=2)

    def rs2_copy(half, d):
        there, to = ring(1 - half, d)
        return remote(summed.at[half, pl.ds(there * 4, 4)], rs2.at[half, d - 1], send_sem.at[5], r_sem.at[2, half, 0], to)

    pairs(0, ring(0, 2)[0])
    pairs(1, ring(1, 2)[0])
    for i in (0, 1):
        far_copy(0, i).start()
        far_copy(1, i).start()
    for i, d in ((0, 3), (1, 1)):
        pairs(0, ring(0, d)[0])
        pairs(1, ring(1, d)[0])
        near_copy(0, i, False).start()
        near_copy(1, i, False).start()
    pairs(0, x)
    pairs(1, z)
    for half in (0, 1):
        for i in (0, 1):
            combine(half, i)
            near_copy(half, i, True).start()

    def out_copy(slot):
        return pltpu.make_async_copy(out_v.at[slot], out.at[0, slot], o_sem)

    live = count[0]

    def energy(position):
        k = slots_s[x, 0, position]
        s = k >> 3
        return ens_s[s & 3, s >> 2, 0, wanted_s[x, k & 7, s]]

    for slot in range(8):
        n = f * 8 + slot
        denom = cabs[...] - (energy(2 * n) + energy(2 * n + 1))
        rec_v[slot] = jnp.where(n < live, 1.0 / denom, 0.0)

    for half in (0, 1):
        me_at = x if half == 0 else z
        for i in (0, 1):
            near_copy(half, i, False).wait_recv()
            near_copy(half, i, True).wait_recv()

        def add(i, carry):
            total = part[half, me_at, i].astype(F32)
            for d in (0, 1):
                total = total + rs_near[half, d, i].astype(F32)
            summed[half, i] = total.astype(BF16)
            return carry

        lax.fori_loop(0, 16, add, 0, unroll=2)
        for d in (2, 1, 3):
            rs2_copy(half, d).start()

    for half in (0, 1):
        me_at = z if half == 0 else x
        remote(rs2.at[half], rs2.at[half], send_sem.at[5], r_sem.at[2, half, 0], me_partner).wait_recv()

        for i in range(4):
            total = summed[half, me_at * 4 + i].astype(F32)
            for d in (0, 1, 2):
                total = total + rs2[half, d, i].astype(F32)
            exchange = total.astype(BF16)
            slot = half * 4 + i
            for at in range(0, 1024, 256):
                at = pl.ds(at, 256)
                weighted = jnp.dot(exchange, coupling[:, at], preferred_element_type=F32)
                out_v[slot, :, at] = (weighted * rec_v[slot, :, at]).astype(BF16)
            if slot:
                out_copy(slot - 1).start()
    out_copy(7).start()

    sent(b_v.at[pl.ds(0, 3)], send_sem.at[4])
    sent(rs2, send_sem.at[5])
    pltpu.make_async_copy(out_v, out.at[0], o_sem).wait()


def on_device(fac, tri, send_map, pair_slots, pair_count, orbital_energy, cabs_energy, coupling):
    dma = pltpu.SemaphoreType.DMA
    ens = jnp.broadcast_to(orbital_energy.astype(F32)[None, :], (8, 16))
    hbm = pl.BlockSpec(memory_space=pl.ANY)
    vmem = pl.BlockSpec(memory_space=pltpu.VMEM)
    return pl.pallas_call(
        fused_kernel,
        out_shape=jax.ShapeDtypeStruct((1, 8, LANES, 1024), BF16),
        in_specs=[hbm, hbm, hbm, hbm, hbm, vmem, vmem, pl.BlockSpec(memory_space=pltpu.SMEM)],
        out_specs=hbm,
        scratch_shapes=[
            pltpu.VMEM((2 * PANEL, 4096), BF16),
            pltpu.VMEM((CHUNKS, 4096, LANES), BF16),
            pltpu.VMEM((CHUNKS, 4, LANES, QROWS), BF16),
            pltpu.VMEM((256, LANES, QROWS), BF16),
            pltpu.VMEM((2, 4, 16, LANES, LANES), BF16),
            pltpu.VMEM((2, 2, 8, LANES, LANES), BF16),
            pltpu.VMEM((2, 2, 16, LANES, LANES), BF16),
            pltpu.VMEM((2, 16, LANES, LANES), BF16),
            pltpu.VMEM((2, 3, 4, LANES, LANES), BF16),
            pltpu.VMEM((4, 8, 16), jnp.int32),
            pltpu.VMEM((4, 1, LANES), jnp.int32),
            pltpu.VMEM((4, 4, 8, 16), F32),
            pltpu.SMEM((4, 8, 16), jnp.int32),
            pltpu.SMEM((4, 1, LANES), jnp.int32),
            pltpu.SMEM((4, 4, 8, 16), F32),
            pltpu.VMEM((8, 1, 1024), F32),
            pltpu.VMEM((8, LANES, 1024), BF16),
            dma((6,)),
            dma((3,)),
            dma((CHUNKS, 3)),
            dma((CHUNKS, 3)),
            dma((CHUNKS, 7)),
            dma,
            dma((4, 4)),
            dma((2, 7)),
            dma((3, 2, 4)),
            dma,
            dma,
        ],
        compiler_params=pltpu.CompilerParams(
            collective_id=0, has_side_effects=True, vmem_limit_bytes=64 * 1024 * 1024 - 65536
        ),
        name="fit_exchange",
    )(fac, tri, jnp.swapaxes(send_map, 1, 2), pair_slots, ens, cabs_energy.reshape(1, 1024), coupling, pair_count)


def solution(mesh):
    in_specs = (
        P("fit", None),
        P("fit", "pair"),
        P("pair", None, None),
        P("pair", None),
        P("pair"),
        P("pair"),
        P(),
        P(),
    )
    return jax.shard_map(
        on_device, mesh=mesh, in_specs=in_specs, out_specs=P("pair", "fit", None, None), check_vma=False
    )
```

```python
import jax
import jax.numpy as jnp
from jax import lax
from jax.experimental import pallas as pl
from jax.experimental.pallas import tpu as pltpu
from jax.sharding import PartitionSpec as P

MESH = pl.DeviceIdType.MESH
F32 = jnp.float32
BF16 = jnp.bfloat16
CHUNKS = 8
LANES = 128
PANEL = 512
QROWS = 256
SCALE = 4096.0 ** -0.5
VMEM_LIMIT = 48 * 1024 * 1024


def fused_kernel(
    fac, tri, wanted, slots, ens, cabs_hbm, coupling_hbm, count,
    out,
    a_v, b_v, f_v, cols, part, rs_far, rs_near, summed, rs2,
    wanted_v, slots_v, ens_v, wanted_s, slots_s, ens_s, rec_v, cabs, coupling,
    send_sem, a_sem, zr, xr, yr, pr, i_sem, e_sem, r_sem, l_sem, o_sem,
):
    f = lax.axis_index("fit")
    p = lax.axis_index("pair")
    z, c = f // 2, f % 2
    x, y = p // 4, p % 4
    nc = 1 - c
    zp, zm, zo = (z + 1) % 4, (z + 3) % 4, (z + 2) % 4
    yp, ym, yo = (y + 1) % 4, (y + 3) % 4, (y + 2) % 4

    def dev(zz, cc, xx, yy):
        return (2 * zz + cc, 4 * xx + yy)

    me_partner = dev(z, nc, x, y)

    def remote(src, dst, ss, rs, to):
        return pltpu.make_async_remote_copy(
            src_ref=src, dst_ref=dst, send_sem=ss, recv_sem=rs, device_id=to, device_id_type=MESH
        )

    barrier = pltpu.get_barrier_semaphore()
    greeted = [me_partner]
    for d in (1, 2, 3):
        greeted.append(dev((z + d) % 4, c, x, y))
        greeted.append(dev(z, c, (x + d) % 4, y))
        greeted.append(dev(z, c, x, (y + d) % 4))
    greeted.append(dev(zp, nc, x, y))
    greeted.append(dev(zm, nc, x, y))
    for to in greeted:
        pl.semaphore_signal(barrier, inc=1, device_id=to, device_id_type=MESH)

    def own_src(h, g):
        return tri.at[:, pl.ds(pl.multiple_of((h * CHUNKS + g) * LANES, LANES), LANES)]

    def panel(g, k):
        return b_v.at[g, pl.ds(pl.multiple_of(k * PANEL, PANEL), PANEL), :]

    def own_first(g):
        return (
            remote(own_src(c, g), panel(g, f), send_sem.at[0], zr.at[g, 0], dev(zp, c, x, y)),
            remote(own_src(c, g), panel(g, f), send_sem.at[0], zr.at[g, 2], dev(zm, c, x, y)),
        )

    def own_second(g):
        return (
            remote(own_src(nc, g), panel(g, f), send_sem.at[0], zr.at[g, 2], dev(zp, nc, x, y)),
            remote(own_src(nc, g), panel(g, f), send_sem.at[0], zr.at[g, 1], dev(zm, nc, x, y)),
            remote(own_src(nc, g), panel(g, f), send_sem.at[0], zr.at[g, 2], me_partner),
        )

    def start(copies):
        for cp in copies:
            cp.start()

    def own_local(g):
        return pltpu.make_async_copy(own_src(c, g), panel(g, f), l_sem)

    def z_forward(g, way):
        k = 2 * zm + c if way == 0 else 2 * zp + nc
        return remote(panel(g, k), panel(g, k), send_sem.at[0], zr.at[g, 2], dev(zp if way == 0 else zm, c, x, y))

    def z_wait(g, i):
        blk = b_v.at[g, pl.ds(0, PANEL if i < 2 else 5 * PANEL), :]
        remote(blk, blk, send_sem.at[0], zr.at[g, i], me_partner).wait_recv()

    def col_at(cc, yy, g):
        return ((cc * 4 + yy) * CHUNKS + g) * 4

    def x_copy(g, i):
        to = (x + 3 - i) % 4
        return remote(f_v.at[g, to], cols.at[col_at(c, y, g) + x], send_sem.at[1], xr.at[g, i], dev(z, c, to, y))

    def x_wait(g, i):
        at = cols.at[col_at(c, y, g)]
        remote(at, at, send_sem.at[1], xr.at[g, i], me_partner).wait_recv()

    def block(at, size):
        return cols.at[pl.ds(at, size)]

    def to_partner(g, yy):
        blk = block(col_at(c, yy, g), 4)
        return remote(blk, blk, send_sem.at[3], pr, me_partner)

    def y_copy(g, way, i):
        blk = cols.at[col_at(c, y, g) + (x + 1 + i) % 4]
        j = ((4, 1, 4, 0), (2, 5, 3, 5))[way][i]
        return remote(blk, blk, send_sem.at[2], yr.at[g, j], dev(z, c, x, yp if way == 0 else ym))

    def y_start(g, i):
        y_copy(g, 0, i).start()
        y_copy(g, 1, i).start()

    def y_forward(g, i):
        yy, to = (ym, yp) if i % 2 else (yp, ym)
        blk = cols.at[col_at(c, yy, g) + (x + 1 + i) % 4]
        return remote(blk, blk, send_sem.at[2], yr.at[g, 6], dev(z, c, x, to))

    def y_wait(g, j):
        blk = block(col_at(c, y, g), (1, 1, 1, 1, 2, 2, 4)[j])
        remote(blk, blk, send_sem.at[2], yr.at[g, j], me_partner).wait_recv()

    def ints_copies():
        out = []
        for i, d in enumerate((1, 2, 3)):
            to = dev(z, c, (x + d) % 4, y)
            out.append(remote(wanted.at[0], wanted_v.at[x], i_sem.at[0, i], i_sem.at[1, i], to))
            out.append(remote(slots, slots_v.at[x], i_sem.at[2, i], i_sem.at[3, i], to))
        return out

    def ens_copies_x():
        return [
            remote(ens, ens_v.at[y, x], e_sem.at[0, i], e_sem.at[1, i], dev(z, c, (x + d) % 4, y))
            for i, d in enumerate((1, 2, 3))
        ]

    def ens_copies_y():
        return [
            remote(ens_v.at[y], ens_v.at[y], e_sem.at[0, 3 + i], e_sem.at[1, 3 + i], dev(z, c, x, (y + d) % 4))
            for i, d in enumerate((1, 2, 3))
        ]

    a_rows = a_v.at[pl.ds(pl.multiple_of(c * PANEL, PANEL), PANEL), :]
    a_partner = remote(fac, a_rows, a_sem.at[0], a_sem.at[1], me_partner)
    a_local = pltpu.make_async_copy(fac, a_rows, a_sem.at[2])
    small_local = (
        pltpu.make_async_copy(wanted.at[0], wanted_v.at[x], i_sem.at[0, 3]),
        pltpu.make_async_copy(slots, slots_v.at[x], i_sem.at[1, 3]),
        pltpu.make_async_copy(ens, ens_v.at[y, x], e_sem.at[0, 6]),
        pltpu.make_async_copy(cabs_hbm, cabs, o_sem.at[0]),
        pltpu.make_async_copy(coupling_hbm, coupling, o_sem.at[1]),
    )

    for g in range(CHUNKS):
        own_local(g).start()
    a_local.start()
    for cp in small_local:
        cp.start()

    pl.semaphore_wait(barrier, len(greeted))

    @pl.when(c == 0)
    def _():
        start(own_first(0))
        start(own_second(0))

    @pl.when(c == 1)
    def _():
        start(own_second(0))
        start(own_first(0))

    a_partner.start()
    for cp in ints_copies() + ens_copies_x():
        cp.start()

    def step(t, carry):
        @pl.when(t < CHUNKS)
        def _():
            z_wait(t, 0)
            z_forward(t, 0).start()
            z_wait(t, 1)
            z_forward(t, 1).start()

        @pl.when(c == 0)
        def _():
            @pl.when(t == 0)
            def _():
                start(own_first(1))

            @pl.when(t < CHUNKS - 1)
            def _():
                start(own_second(t + 1))

            @pl.when(t < CHUNKS - 2)
            def _():
                start(own_first(t + 2))

        @pl.when(c == 1)
        def _():
            @pl.when(t == 0)
            def _():
                start(own_second(1))

            @pl.when(t < CHUNKS - 1)
            def _():
                start(own_first(t + 1))

            @pl.when(t < CHUNKS - 2)
            def _():
                start(own_second(t + 2))

        def send_rest(g):
            for i in (0, 2, 1):
                x_wait(g, i)
                y_start(g, i)
            to_partner(g, y).start()

        @pl.when((t == 1) | ((t >= 3) & (t < CHUNKS)))
        def _():
            send_rest(jnp.maximum(t - 2, 0))

        @pl.when((t == 0) | ((t >= 2) & (t < CHUNKS + 1)))
        def _():
            g = jnp.maximum(t - 1, 0)

            @pl.when(t == 0)
            def _():
                a_partner.wait_recv()
                a_local.wait()
                pltpu.make_async_copy(b_v.at[0], b_v.at[0], l_sem).wait()

            z_wait(g, 2)

            def fit(q):
                rows = pl.ds(pl.multiple_of(q * QROWS, QROWS), QROWS)
                acc = jnp.dot(a_v[rows, :], b_v[g], preferred_element_type=F32)
                return acc.T.astype(BF16)

            cols[col_at(c, y, g) + x] = fit(x)

            def fit_send(j, carry):
                i = jnp.where(j < 2, 1 - j, 2)
                q = (x + 3 - i) % 4
                f_v[g, q] = fit(q)
                x_copy(g, i).start()

                @pl.when(j == 0)
                def _():
                    y_start(g, 3)

                return carry

            lax.fori_loop(0, 3, fit_send, 0)

        @pl.when(t == CHUNKS)
        def _():
            send_rest(CHUNKS - 2)

        @pl.when((t >= 3) & (t < CHUNKS + 3))
        def _():
            g = t - 3
            for j, i in ((0, 3), (2, 0), (3, 2), (1, 1)):
                y_wait(g, j)
                y_forward(g, i).start()
            y_wait(g, 4)
            y_wait(g, 5)
            to_partner(g, ym).start()
            to_partner(g, yp).start()

        @pl.when(t == CHUNKS)
        def _():
            send_rest(CHUNKS - 1)

        @pl.when(t >= 4)
        def _():
            y_wait(t - 4, 6)
            to_partner(t - 4, yo).start()

        @pl.when(t == 2)
        def _():
            for cp in ints_copies() + ens_copies_x():
                cp.wait()
            for cp in small_local:
                cp.wait()
            for cp in ens_copies_y():
                cp.start()

        @pl.when(t == 6)
        def _():
            for cp in ens_copies_y():
                cp.wait()
            to_smem = (
                pltpu.make_async_copy(wanted_v, wanted_s, i_sem.at[2, 3]),
                pltpu.make_async_copy(slots_v, slots_s, i_sem.at[3, 3]),
                pltpu.make_async_copy(ens_v, ens_s, e_sem.at[1, 6]),
            )
            for cp in to_smem:
                cp.start()
            for cp in to_smem:
                cp.wait()

        return carry

    lax.fori_loop(0, CHUNKS + 4, step, 0)

    def sent(ref, sem):
        remote(ref, ref, sem, pr, me_partner).wait_send()

    remote(b_v, b_v, send_sem.at[3], pr, me_partner).wait_recv()
    sent(b_v.at[pl.ds(0, 7)], send_sem.at[0])
    sent(f_v.at[pl.ds(0, 6)], send_sem.at[1])
    sent(b_v.at[pl.ds(0, 6)], send_sem.at[2])
    sent(b_v, send_sem.at[3])
    a_partner.wait_send()

    def orbital(xo, position):
        k = slots_s[xo, 0, position]
        s = k >> 3
        t = wanted_s[xo, k & 7, s]
        return ((t >> 3) << 7) + ((s & 3) << 5) + ((t & 7) << 2) + (s >> 2)

    def pairs(half, first):
        def some(j, carry):
            done = []
            for slot in range(8):
                second = 2 * j + slot // 4
                xo, zz = (first, second) if half == 0 else (second, first)
                n = (2 * zz + c) * 8 + half * 4 + slot % 4
                left = cols[orbital(xo, 2 * n)]
                right = cols[orbital(xo, 2 * n + 1)]
                e = lax.dot_general(left, right, (((1,), (1,)), ((), ())), preferred_element_type=F32)
                done.append((e * SCALE).astype(BF16))
            for slot in range(8):
                part[half, first, j * 8 + slot] = done[slot]
            return carry

        lax.fori_loop(0, 2, some, 0)

    def ring(half, d):
        if half == 0:
            at = (x + d) % 4
            return at, dev(z, c, at, y)
        at = (z + d) % 4
        return at, dev(at, c, x, y)

    def far_copy(half, i):
        far, _ = ring(half, 2)
        _, to = ring(half, 3 if i == 0 else 1)
        return remote(part.at[half, far, pl.ds(8 * i, 8)], rs_far.at[half, i], send_sem.at[4], r_sem.at[0, half, i], to)

    def near_copy(half, i, summed_part):
        at, to = ring(half, 3 if i == 0 else 1)
        first = 8 * i if summed_part else 8 - 8 * i
        j = 2 * i + (1 if summed_part else 0)
        rows = pl.ds(first, 8)
        return remote(part.at[half, at, rows], rs_near.at[half, i, rows], send_sem.at[4], r_sem.at[1, half, j], to)

    def combine(half, i):
        at, _ = ring(half, 3 if i == 0 else 1)
        far_copy(half, i).wait_recv()

        def add(k, carry):
            part[half, at, 8 * i + k] = (part[half, at, 8 * i + k].astype(F32) + rs_far[half, i, k].astype(F32)).astype(BF16)
            return carry

        lax.fori_loop(0, 8, add, 0, unroll=2)

    def rs2_copy(half, d):
        there, to = ring(1 - half, d)
        return remote(summed.at[half, pl.ds(there * 4, 4)], rs2.at[half, d - 1], send_sem.at[5], r_sem.at[2, half, 0], to)

    pairs(0, ring(0, 2)[0])
    pairs(1, ring(1, 2)[0])
    for i in (0, 1):
        far_copy(0, i).start()
        far_copy(1, i).start()
    for i, d in ((0, 3), (1, 1)):
        pairs(0, ring(0, d)[0])
        pairs(1, ring(1, d)[0])
        near_copy(0, i, False).start()
        near_copy(1, i, False).start()
    pairs(0, x)
    pairs(1, z)
    for half in (0, 1):
        for i in (0, 1):
            combine(half, i)
            near_copy(half, i, True).start()

    live = count[0]

    def energy(position):
        k = slots_s[x, 0, position]
        s = k >> 3
        return ens_s[s & 3, s >> 2, 0, wanted_s[x, k & 7, s]]

    for slot in range(8):
        n = f * 8 + slot
        denom = cabs[...] - (energy(2 * n) + energy(2 * n + 1))
        rec_v[slot] = jnp.where(n < live, 1.0 / denom, 0.0)

    for half in (0, 1):
        me_at = x if half == 0 else z
        for i in (0, 1):
            near_copy(half, i, False).wait_recv()
            near_copy(half, i, True).wait_recv()

        def add(i, carry):
            total = part[half, me_at, i].astype(F32)
            for d in (0, 1):
                total = total + rs_near[half, d, i].astype(F32)
            summed[half, i] = total.astype(BF16)
            return carry

        lax.fori_loop(0, 16, add, 0, unroll=2)
        for d in (2, 1, 3):
            rs2_copy(half, d).start()

    for half in (0, 1):
        me_at = z if half == 0 else x
        remote(rs2.at[half], rs2.at[half], send_sem.at[5], r_sem.at[2, half, 0], me_partner).wait_recv()

        for i in range(4):
            total = summed[half, me_at * 4 + i].astype(F32)
            for d in (0, 1, 2):
                total = total + rs2[half, d, i].astype(F32)
            exchange = total.astype(BF16)
            slot = half * 4 + i
            for at in range(0, 1024, 256):
                at = pl.ds(at, 256)
                weighted = jnp.dot(exchange, coupling[:, at], preferred_element_type=F32)
                out[0, slot, :, at] = (weighted * rec_v[slot, :, at]).astype(BF16)

    sent(b_v.at[pl.ds(0, 3)], send_sem.at[4])
    sent(rs2, send_sem.at[5])


def on_device(fac, tri, send_map, pair_slots, pair_count, orbital_energy, cabs_energy, coupling):
    dma = pltpu.SemaphoreType.DMA
    ens = jnp.broadcast_to(orbital_energy.astype(F32)[None, :], (8, 16))
    hbm = pl.BlockSpec(memory_space=pltpu.HBM)
    vmem = pl.BlockSpec(memory_space=pltpu.VMEM)
    return pl.pallas_call(
        fused_kernel,
        out_shape=jax.ShapeDtypeStruct((1, 8, LANES, 1024), BF16),
        in_specs=[hbm, hbm, hbm, hbm, hbm, hbm, hbm, pl.BlockSpec(memory_space=pltpu.SMEM)],
        out_specs=vmem,
        scratch_shapes=[
            pltpu.VMEM((2 * PANEL, 4096), BF16),
            pltpu.VMEM((CHUNKS, 4096, LANES), BF16),
            pltpu.VMEM((CHUNKS, 4, LANES, QROWS), BF16),
            pltpu.VMEM((256, LANES, QROWS), BF16),
            pltpu.VMEM((2, 4, 16, LANES, LANES), BF16),
            pltpu.VMEM((2, 2, 8, LANES, LANES), BF16),
            pltpu.VMEM((2, 2, 16, LANES, LANES), BF16),
            pltpu.VMEM((2, 16, LANES, LANES), BF16),
            pltpu.VMEM((2, 3, 4, LANES, LANES), BF16),
            pltpu.VMEM((4, 8, 16), jnp.int32),
            pltpu.VMEM((4, 1, LANES), jnp.int32),
            pltpu.VMEM((4, 4, 8, 16), F32),
            pltpu.SMEM((4, 8, 16), jnp.int32),
            pltpu.SMEM((4, 1, LANES), jnp.int32),
            pltpu.SMEM((4, 4, 8, 16), F32),
            pltpu.VMEM((8, 1, 1024), F32),
            pltpu.VMEM((1, 1024), F32),
            pltpu.VMEM((LANES, 1024), BF16),
            dma((6,)),
            dma((3,)),
            dma((CHUNKS, 3)),
            dma((CHUNKS, 3)),
            dma((CHUNKS, 7)),
            dma,
            dma((4, 4)),
            dma((2, 7)),
            dma((3, 2, 4)),
            dma,
            dma((2,)),
        ],
        compiler_params=pltpu.CompilerParams(
            collective_id=0, has_side_effects=True, vmem_limit_bytes=VMEM_LIMIT
        ),
        name="fit_exchange",
    )(
        *(
            pltpu.with_memory_space_constraint(a, pltpu.HBM)
            for a in (fac, tri, jnp.swapaxes(send_map, 1, 2), pair_slots, ens, cabs_energy.reshape(1, 1024), coupling)
        ),
        pair_count,
    )


def solution(mesh):
    in_specs = (
        P("fit", None),
        P("fit", "pair"),
        P("pair", None, None),
        P("pair", None),
        P("pair"),
        P("pair"),
        P(),
        P(),
    )
    return jax.shard_map(
        on_device, mesh=mesh, in_specs=in_specs, out_specs=P("pair", "fit", None, None), check_vma=False
    )
```

```python
import jax
import jax.numpy as jnp
from jax import lax
from jax.experimental import pallas as pl
from jax.experimental.pallas import tpu as pltpu
from jax.sharding import PartitionSpec as P

MESH = pl.DeviceIdType.MESH
F32 = jnp.float32
BF16 = jnp.bfloat16
CHUNKS = 8
LANES = 128
PANEL = 512
QROWS = 256
SCALE = 4096.0 ** -0.5
VMEM_LIMIT = 48 * 1024 * 1024


def fused_kernel(
    fac, tri, wanted, slots, ens, cabs_hbm, coupling_hbm, count,
    out,
    a_v, b_v, f_v, cols, part, rs_far, rs_near, summed, rs2,
    wanted_v, slots_v, ens_v, wanted_s, slots_s, ens_s, rec_v, cabs, coupling,
    send_sem, a_sem, zr, xr, yr, pr, i_sem, e_sem, r_sem, l_sem, o_sem,
):
    f = lax.axis_index("fit")
    p = lax.axis_index("pair")
    z, c = f // 2, f % 2
    x, y = p // 4, p % 4
    nc = 1 - c
    zp, zm, zo = (z + 1) % 4, (z + 3) % 4, (z + 2) % 4
    yp, ym, yo = (y + 1) % 4, (y + 3) % 4, (y + 2) % 4

    def dev(zz, cc, xx, yy):
        return (2 * zz + cc, 4 * xx + yy)

    me_partner = dev(z, nc, x, y)

    def remote(src, dst, ss, rs, to):
        return pltpu.make_async_remote_copy(
            src_ref=src, dst_ref=dst, send_sem=ss, recv_sem=rs, device_id=to, device_id_type=MESH
        )

    barrier = pltpu.get_barrier_semaphore()
    greeted = [me_partner]
    for d in (1, 2, 3):
        greeted.append(dev((z + d) % 4, c, x, y))
        greeted.append(dev(z, c, (x + d) % 4, y))
        greeted.append(dev(z, c, x, (y + d) % 4))
    greeted.append(dev(zp, nc, x, y))
    greeted.append(dev(zm, nc, x, y))
    for to in greeted:
        pl.semaphore_signal(barrier, inc=1, device_id=to, device_id_type=MESH)

    def own_src(h, g):
        return tri.at[:, pl.ds(pl.multiple_of((h * CHUNKS + g) * LANES, LANES), LANES)]

    def panel(g, k):
        return b_v.at[g, pl.ds(pl.multiple_of(k * PANEL, PANEL), PANEL), :]

    def own_first(g):
        return (
            remote(own_src(c, g), panel(g, f), send_sem.at[0], zr.at[g, 0], dev(zp, c, x, y)),
            remote(own_src(c, g), panel(g, f), send_sem.at[0], zr.at[g, 2], dev(zm, c, x, y)),
        )

    def own_second(g):
        return (
            remote(own_src(nc, g), panel(g, f), send_sem.at[0], zr.at[g, 2], dev(zp, nc, x, y)),
            remote(own_src(nc, g), panel(g, f), send_sem.at[0], zr.at[g, 1], dev(zm, nc, x, y)),
            remote(own_src(nc, g), panel(g, f), send_sem.at[0], zr.at[g, 2], me_partner),
        )

    def start(copies):
        for cp in copies:
            cp.start()

    def own_local(g):
        return pltpu.make_async_copy(own_src(c, g), panel(g, f), l_sem)

    def z_forward(g, way):
        k = 2 * zm + c if way == 0 else 2 * zp + nc
        return remote(panel(g, k), panel(g, k), send_sem.at[0], zr.at[g, 2], dev(zp if way == 0 else zm, c, x, y))

    def z_wait(g, i):
        blk = b_v.at[g, pl.ds(0, PANEL if i < 2 else 5 * PANEL), :]
        remote(blk, blk, send_sem.at[0], zr.at[g, i], me_partner).wait_recv()

    def col_at(cc, yy, g):
        return ((cc * 4 + yy) * CHUNKS + g) * 4

    def x_copy(g, i):
        to = (x + 3 - i) % 4
        return remote(f_v.at[g, to], cols.at[col_at(c, y, g) + x], send_sem.at[1], xr.at[g, i], dev(z, c, to, y))

    def x_wait(g, i):
        at = cols.at[col_at(c, y, g)]
        remote(at, at, send_sem.at[1], xr.at[g, i], me_partner).wait_recv()

    def block(at, size):
        return cols.at[pl.ds(at, size)]

    def to_partner(g, yy):
        blk = block(col_at(c, yy, g), 4)
        return remote(blk, blk, send_sem.at[3], pr, me_partner)

    def y_copy(g, way, i):
        blk = cols.at[col_at(c, y, g) + (x + 1 + i) % 4]
        j = ((4, 1, 4, 0), (2, 5, 3, 5))[way][i]
        return remote(blk, blk, send_sem.at[2], yr.at[g, j], dev(z, c, x, yp if way == 0 else ym))

    def y_start(g, i):
        y_copy(g, 0, i).start()
        y_copy(g, 1, i).start()

    def y_forward(g, i):
        yy, to = (ym, yp) if i % 2 else (yp, ym)
        blk = cols.at[col_at(c, yy, g) + (x + 1 + i) % 4]
        return remote(blk, blk, send_sem.at[2], yr.at[g, 6], dev(z, c, x, to))

    def y_wait(g, j):
        blk = block(col_at(c, y, g), (1, 1, 1, 1, 2, 2, 4)[j])
        remote(blk, blk, send_sem.at[2], yr.at[g, j], me_partner).wait_recv()

    def ints_copies():
        out = []
        for i, d in enumerate((1, 2, 3)):
            to = dev(z, c, (x + d) % 4, y)
            out.append(remote(wanted.at[0], wanted_v.at[x], i_sem.at[0, i], i_sem.at[1, i], to))
            out.append(remote(slots, slots_v.at[x], i_sem.at[2, i], i_sem.at[3, i], to))
        return out

    def ens_copies_x():
        return [
            remote(ens, ens_v.at[y, x], e_sem.at[0, i], e_sem.at[1, i], dev(z, c, (x + d) % 4, y))
            for i, d in enumerate((1, 2, 3))
        ]

    def ens_copies_y():
        return [
            remote(ens_v.at[y], ens_v.at[y], e_sem.at[0, 3 + i], e_sem.at[1, 3 + i], dev(z, c, x, (y + d) % 4))
            for i, d in enumerate((1, 2, 3))
        ]

    a_rows = a_v.at[pl.ds(pl.multiple_of(c * PANEL, PANEL), PANEL), :]
    a_partner = remote(fac, a_rows, a_sem.at[0], a_sem.at[1], me_partner)
    a_local = pltpu.make_async_copy(fac, a_rows, a_sem.at[2])
    small_local = (
        pltpu.make_async_copy(wanted.at[0], wanted_v.at[x], i_sem.at[0, 3]),
        pltpu.make_async_copy(slots, slots_v.at[x], i_sem.at[1, 3]),
        pltpu.make_async_copy(ens, ens_v.at[y, x], e_sem.at[0, 6]),
        pltpu.make_async_copy(cabs_hbm, cabs, o_sem.at[0]),
        pltpu.make_async_copy(coupling_hbm, coupling, o_sem.at[1]),
    )

    for g in range(CHUNKS):
        own_local(g).start()
    a_local.start()
    for cp in small_local:
        cp.start()

    pl.semaphore_wait(barrier, len(greeted))

    @pl.when(c == 0)
    def _():
        start(own_first(0))
        start(own_second(0))

    @pl.when(c == 1)
    def _():
        start(own_second(0))
        start(own_first(0))

    a_partner.start()
    for cp in ints_copies() + ens_copies_x():
        cp.start()

    def step(t, carry):
        @pl.when(t < CHUNKS)
        def _():
            z_wait(t, 0)
            z_forward(t, 0).start()
            z_wait(t, 1)
            z_forward(t, 1).start()

        @pl.when(c == 0)
        def _():
            @pl.when(t == 0)
            def _():
                start(own_first(1))

            @pl.when(t < CHUNKS - 1)
            def _():
                start(own_second(t + 1))

            @pl.when(t < CHUNKS - 2)
            def _():
                start(own_first(t + 2))

        @pl.when(c == 1)
        def _():
            @pl.when(t == 0)
            def _():
                start(own_second(1))

            @pl.when(t < CHUNKS - 1)
            def _():
                start(own_first(t + 1))

            @pl.when(t < CHUNKS - 2)
            def _():
                start(own_second(t + 2))

        def send_rest(g):
            for i in (0, 2, 1):
                x_wait(g, i)
                y_start(g, i)
            to_partner(g, y).start()

        @pl.when((t == 1) | ((t >= 3) & (t < CHUNKS)))
        def _():
            send_rest(jnp.maximum(t - 2, 0))

        @pl.when((t == 0) | ((t >= 2) & (t < CHUNKS + 1)))
        def _():
            g = jnp.maximum(t - 1, 0)

            @pl.when(t == 0)
            def _():
                a_partner.wait_recv()
                a_local.wait()
                pltpu.make_async_copy(b_v.at[0], b_v.at[0], l_sem).wait()

            z_wait(g, 2)

            def fit(q):
                rows = pl.ds(pl.multiple_of(q * QROWS, QROWS), QROWS)
                acc = jnp.dot(a_v[rows, :], b_v[g], preferred_element_type=F32)
                return acc.T.astype(BF16)

            cols[col_at(c, y, g) + x] = fit(x)

            def fit_send(j, carry):
                i = jnp.where(j < 2, 1 - j, 2)
                q = (x + 3 - i) % 4
                f_v[g, q] = fit(q)
                x_copy(g, i).start()

                @pl.when(j == 0)
                def _():
                    y_start(g, 3)

                return carry

            lax.fori_loop(0, 3, fit_send, 0)

        @pl.when(t == CHUNKS)
        def _():
            send_rest(CHUNKS - 2)

        @pl.when((t >= 3) & (t < CHUNKS + 3))
        def _():
            g = t - 3
            for j, i in ((0, 3), (2, 0), (3, 2), (1, 1)):
                y_wait(g, j)
                y_forward(g, i).start()
            y_wait(g, 4)
            y_wait(g, 5)
            to_partner(g, ym).start()
            to_partner(g, yp).start()

        @pl.when(t == CHUNKS)
        def _():
            send_rest(CHUNKS - 1)

        @pl.when(t >= 4)
        def _():
            y_wait(t - 4, 6)
            to_partner(t - 4, yo).start()

        @pl.when(t == 2)
        def _():
            for cp in ints_copies() + ens_copies_x():
                cp.wait()
            for cp in small_local:
                cp.wait()
            for cp in ens_copies_y():
                cp.start()

        @pl.when(t == 6)
        def _():
            for cp in ens_copies_y():
                cp.wait()
            to_smem = (
                pltpu.make_async_copy(wanted_v, wanted_s, i_sem.at[2, 3]),
                pltpu.make_async_copy(slots_v, slots_s, i_sem.at[3, 3]),
                pltpu.make_async_copy(ens_v, ens_s, e_sem.at[1, 6]),
            )
            for cp in to_smem:
                cp.start()
            for cp in to_smem:
                cp.wait()

        return carry

    lax.fori_loop(0, CHUNKS + 4, step, 0)

    def sent(ref, sem):
        remote(ref, ref, sem, pr, me_partner).wait_send()

    remote(b_v, b_v, send_sem.at[3], pr, me_partner).wait_recv()
    sent(b_v.at[pl.ds(0, 7)], send_sem.at[0])
    sent(f_v.at[pl.ds(0, 6)], send_sem.at[1])
    sent(b_v.at[pl.ds(0, 6)], send_sem.at[2])
    sent(b_v, send_sem.at[3])
    a_partner.wait_send()

    def orbital(xo, position):
        k = slots_s[xo, 0, position]
        s = k >> 3
        t = wanted_s[xo, k & 7, s]
        return ((t >> 3) << 7) + ((s & 3) << 5) + ((t & 7) << 2) + (s >> 2)

    def pairs(half, first, steps=(0, 2)):
        def some(j, carry):
            done = []
            for slot in range(8):
                second = 2 * j + slot // 4
                xo, zz = (first, second) if half == 0 else (second, first)
                n = (2 * zz + c) * 8 + half * 4 + slot % 4
                left = cols[orbital(xo, 2 * n)]
                right = cols[orbital(xo, 2 * n + 1)]
                e = lax.dot_general(left, right, (((1,), (1,)), ((), ())), preferred_element_type=F32)
                done.append((e * SCALE).astype(BF16))
            for slot in range(8):
                part[half, first, j * 8 + slot] = done[slot]
            return carry

        lax.fori_loop(*steps, some, 0)

    def ring(half, d):
        if half == 0:
            at = (x + d) % 4
            return at, dev(z, c, at, y)
        at = (z + d) % 4
        return at, dev(at, c, x, y)

    def far_copy(half, i):
        far, _ = ring(half, 2)
        _, to = ring(half, 3 if i == 0 else 1)
        return remote(part.at[half, far, pl.ds(8 * i, 8)], rs_far.at[half, i], send_sem.at[4], r_sem.at[0, half, i], to)

    def near_copy(half, i, summed_part):
        at, to = ring(half, 3 if i == 0 else 1)
        first = 8 * i if summed_part else 8 - 8 * i
        j = 2 * i + (1 if summed_part else 0)
        rows = pl.ds(first, 8)
        return remote(part.at[half, at, rows], rs_near.at[half, i, rows], send_sem.at[4], r_sem.at[1, half, j], to)

    def combine(half, i):
        at, _ = ring(half, 3 if i == 0 else 1)
        far_copy(half, i).wait_recv()

        def add(k, carry):
            part[half, at, 8 * i + k] = (part[half, at, 8 * i + k].astype(F32) + rs_far[half, i, k].astype(F32)).astype(BF16)
            return carry

        lax.fori_loop(0, 8, add, 0, unroll=2)

    def rs2_copy(half, d):
        there, to = ring(1 - half, d)
        return remote(summed.at[half, pl.ds(there * 4, 4)], rs2.at[half, d - 1], send_sem.at[5], r_sem.at[2, half, 0], to)

    last = None
    for i in (0, 1):
        for half in (0, 1):
            pairs(half, ring(half, 2)[0], (i, i + 1))
            if last is not None:
                last.start()
            last = far_copy(half, i)
    last.start()
    for i, d in ((0, 3), (1, 1)):
        pairs(0, ring(0, d)[0])
        pairs(1, ring(1, d)[0])
        near_copy(0, i, False).start()
        near_copy(1, i, False).start()
    pairs(0, x)
    pairs(1, z)
    for half in (0, 1):
        for i in (0, 1):
            combine(half, i)
            near_copy(half, i, True).start()

    live = count[0]

    def energy(position):
        k = slots_s[x, 0, position]
        s = k >> 3
        return ens_s[s & 3, s >> 2, 0, wanted_s[x, k & 7, s]]

    for slot in range(8):
        n = f * 8 + slot
        denom = cabs[...] - (energy(2 * n) + energy(2 * n + 1))
        rec_v[slot] = jnp.where(n < live, 1.0 / denom, 0.0)

    for half in (0, 1):
        me_at = x if half == 0 else z
        for i in (0, 1):
            near_copy(half, i, False).wait_recv()
            near_copy(half, i, True).wait_recv()

        def add(i, carry):
            total = part[half, me_at, i].astype(F32)
            for d in (0, 1):
                total = total + rs_near[half, d, i].astype(F32)
            summed[half, i] = total.astype(BF16)
            return carry

        lax.fori_loop(0, 16, add, 0, unroll=2)
        for d in (2, 1, 3):
            rs2_copy(half, d).start()

    for half in (0, 1):
        me_at = z if half == 0 else x
        remote(rs2.at[half], rs2.at[half], send_sem.at[5], r_sem.at[2, half, 0], me_partner).wait_recv()

        for i in range(4):
            total = summed[half, me_at * 4 + i].astype(F32)
            for d in (0, 1, 2):
                total = total + rs2[half, d, i].astype(F32)
            exchange = total.astype(BF16)
            slot = half * 4 + i
            for at in range(0, 1024, 256):
                at = pl.ds(at, 256)
                weighted = jnp.dot(exchange, coupling[:, at], preferred_element_type=F32)
                out[0, slot, :, at] = (weighted * rec_v[slot, :, at]).astype(BF16)

    sent(b_v.at[pl.ds(0, 3)], send_sem.at[4])
    sent(rs2, send_sem.at[5])


def on_device(fac, tri, send_map, pair_slots, pair_count, orbital_energy, cabs_energy, coupling):
    dma = pltpu.SemaphoreType.DMA
    ens = jnp.broadcast_to(orbital_energy.astype(F32)[None, :], (8, 16))
    hbm = pl.BlockSpec(memory_space=pltpu.HBM)
    vmem = pl.BlockSpec(memory_space=pltpu.VMEM)
    return pl.pallas_call(
        fused_kernel,
        out_shape=jax.ShapeDtypeStruct((1, 8, LANES, 1024), BF16),
        in_specs=[hbm, hbm, hbm, hbm, hbm, hbm, hbm, pl.BlockSpec(memory_space=pltpu.SMEM)],
        out_specs=vmem,
        scratch_shapes=[
            pltpu.VMEM((2 * PANEL, 4096), BF16),
            pltpu.VMEM((CHUNKS, 4096, LANES), BF16),
            pltpu.VMEM((CHUNKS, 4, LANES, QROWS), BF16),
            pltpu.VMEM((256, LANES, QROWS), BF16),
            pltpu.VMEM((2, 4, 16, LANES, LANES), BF16),
            pltpu.VMEM((2, 2, 8, LANES, LANES), BF16),
            pltpu.VMEM((2, 2, 16, LANES, LANES), BF16),
            pltpu.VMEM((2, 16, LANES, LANES), BF16),
            pltpu.VMEM((2, 3, 4, LANES, LANES), BF16),
            pltpu.VMEM((4, 8, 16), jnp.int32),
            pltpu.VMEM((4, 1, LANES), jnp.int32),
            pltpu.VMEM((4, 4, 8, 16), F32),
            pltpu.SMEM((4, 8, 16), jnp.int32),
            pltpu.SMEM((4, 1, LANES), jnp.int32),
            pltpu.SMEM((4, 4, 8, 16), F32),
            pltpu.VMEM((8, 1, 1024), F32),
            pltpu.VMEM((1, 1024), F32),
            pltpu.VMEM((LANES, 1024), BF16),
            dma((6,)),
            dma((3,)),
            dma((CHUNKS, 3)),
            dma((CHUNKS, 3)),
            dma((CHUNKS, 7)),
            dma,
            dma((4, 4)),
            dma((2, 7)),
            dma((3, 2, 4)),
            dma,
            dma((2,)),
        ],
        compiler_params=pltpu.CompilerParams(
            collective_id=0, has_side_effects=True, vmem_limit_bytes=VMEM_LIMIT
        ),
        name="fit_exchange",
    )(
        *(
            pltpu.with_memory_space_constraint(a, pltpu.HBM)
            for a in (fac, tri, jnp.swapaxes(send_map, 1, 2), pair_slots, ens, cabs_energy.reshape(1, 1024), coupling)
        ),
        pair_count,
    )


def solution(mesh):
    in_specs = (
        P("fit", None),
        P("fit", "pair"),
        P("pair", None, None),
        P("pair", None),
        P("pair"),
        P("pair"),
        P(),
        P(),
    )
    return jax.shard_map(
        on_device, mesh=mesh, in_specs=in_specs, out_specs=P("pair", "fit", None, None), check_vma=False
    )
```

```python
import jax
import jax.numpy as jnp
from jax import lax
from jax.experimental import pallas as pl
from jax.experimental.pallas import tpu as pltpu
from jax.sharding import PartitionSpec as P

MESH = pl.DeviceIdType.MESH
F32 = jnp.float32
BF16 = jnp.bfloat16
CHUNKS = 8
LANES = 128
PANEL = 512
QROWS = 256
SCALE = 4096.0 ** -0.5
VMEM_LIMIT = 48 * 1024 * 1024


def fused_kernel(
    fac, tri, wanted, slots, cabs_hbm, coupling_hbm, own_energy, count,
    out,
    a_v, b_v, f_v, cols, part, rs_far, rs_near, summed, rs2,
    wanted_v, slots_v, ens_v, wanted_s, slots_s, ens_s, rec_v, cabs, coupling,
    send_sem, a_sem, zr, xr, yr, pr, i_sem, e_sem, r_sem, l_sem, o_sem,
):
    f = lax.axis_index("fit")
    p = lax.axis_index("pair")
    z, c = f // 2, f % 2
    x, y = p // 4, p % 4
    nc = 1 - c
    zp, zm, zo = (z + 1) % 4, (z + 3) % 4, (z + 2) % 4
    yp, ym, yo = (y + 1) % 4, (y + 3) % 4, (y + 2) % 4

    def dev(zz, cc, xx, yy):
        return (2 * zz + cc, 4 * xx + yy)

    me_partner = dev(z, nc, x, y)

    def remote(src, dst, ss, rs, to):
        return pltpu.make_async_remote_copy(
            src_ref=src, dst_ref=dst, send_sem=ss, recv_sem=rs, device_id=to, device_id_type=MESH
        )

    barrier = pltpu.get_barrier_semaphore()
    greeted = [me_partner]
    for d in (1, 2, 3):
        greeted.append(dev((z + d) % 4, c, x, y))
        greeted.append(dev(z, c, (x + d) % 4, y))
        greeted.append(dev(z, c, x, (y + d) % 4))
    greeted.append(dev(zp, nc, x, y))
    greeted.append(dev(zm, nc, x, y))
    for to in greeted:
        pl.semaphore_signal(barrier, inc=1, device_id=to, device_id_type=MESH)

    def own_src(h, g):
        return tri.at[:, pl.ds(pl.multiple_of((h * CHUNKS + g) * LANES, LANES), LANES)]

    def panel(g, k):
        return b_v.at[g, pl.ds(pl.multiple_of(k * PANEL, PANEL), PANEL), :]

    def own_first(g):
        return (
            remote(own_src(c, g), panel(g, f), send_sem.at[0], zr.at[g, 0], dev(zp, c, x, y)),
            remote(own_src(c, g), panel(g, f), send_sem.at[0], zr.at[g, 2], dev(zm, c, x, y)),
        )

    def own_second(g):
        return (
            remote(own_src(nc, g), panel(g, f), send_sem.at[0], zr.at[g, 2], dev(zp, nc, x, y)),
            remote(own_src(nc, g), panel(g, f), send_sem.at[0], zr.at[g, 1], dev(zm, nc, x, y)),
            remote(own_src(nc, g), panel(g, f), send_sem.at[0], zr.at[g, 2], me_partner),
        )

    def start(copies):
        for cp in copies:
            cp.start()

    def own_local(g):
        return pltpu.make_async_copy(own_src(c, g), panel(g, f), l_sem)

    def z_forward(g, way):
        k = 2 * zm + c if way == 0 else 2 * zp + nc
        return remote(panel(g, k), panel(g, k), send_sem.at[0], zr.at[g, 2], dev(zp if way == 0 else zm, c, x, y))

    def z_wait(g, i):
        blk = b_v.at[g, pl.ds(0, PANEL if i < 2 else 5 * PANEL), :]
        remote(blk, blk, send_sem.at[0], zr.at[g, i], me_partner).wait_recv()

    def col_at(cc, yy, g):
        return ((cc * 4 + yy) * CHUNKS + g) * 4

    def x_copy(g, i):
        to = (x + 3 - i) % 4
        return remote(f_v.at[g, to], cols.at[col_at(c, y, g) + x], send_sem.at[1], xr.at[g, i], dev(z, c, to, y))

    def x_wait(g, i):
        at = cols.at[col_at(c, y, g)]
        remote(at, at, send_sem.at[1], xr.at[g, i], me_partner).wait_recv()

    def block(at, size):
        return cols.at[pl.ds(at, size)]

    def to_partner(g, yy):
        blk = block(col_at(c, yy, g), 4)
        return remote(blk, blk, send_sem.at[3], pr, me_partner)

    def y_copy(g, way, i):
        blk = cols.at[col_at(c, y, g) + (x + 1 + i) % 4]
        j = ((4, 1, 4, 0), (2, 5, 3, 5))[way][i]
        return remote(blk, blk, send_sem.at[2], yr.at[g, j], dev(z, c, x, yp if way == 0 else ym))

    def y_start(g, i):
        y_copy(g, 0, i).start()
        y_copy(g, 1, i).start()

    def y_forward(g, i):
        yy, to = (ym, yp) if i % 2 else (yp, ym)
        blk = cols.at[col_at(c, yy, g) + (x + 1 + i) % 4]
        return remote(blk, blk, send_sem.at[2], yr.at[g, 6], dev(z, c, x, to))

    def y_wait(g, j):
        blk = block(col_at(c, y, g), (1, 1, 1, 1, 2, 2, 4)[j])
        remote(blk, blk, send_sem.at[2], yr.at[g, j], me_partner).wait_recv()

    def ints_copies():
        out = []
        for i, d in enumerate((1, 2, 3)):
            to = dev(z, c, (x + d) % 4, y)
            out.append(remote(wanted.at[0], wanted_v.at[x], i_sem.at[0, i], i_sem.at[1, i], to))
            out.append(remote(slots, slots_v.at[x], i_sem.at[2, i], i_sem.at[3, i], to))
        return out

    def ens_copies_x():
        return [
            remote(ens_v.at[y, x], ens_v.at[y, x], e_sem.at[0, i], e_sem.at[1, i], dev(z, c, (x + d) % 4, y))
            for i, d in enumerate((1, 2, 3))
        ]

    def ens_copies_y():
        return [
            remote(ens_v.at[y], ens_v.at[y], e_sem.at[0, 3 + i], e_sem.at[1, 3 + i], dev(z, c, x, (y + d) % 4))
            for i, d in enumerate((1, 2, 3))
        ]

    a_rows = a_v.at[pl.ds(pl.multiple_of(c * PANEL, PANEL), PANEL), :]
    a_partner = remote(fac, a_rows, a_sem.at[0], a_sem.at[1], me_partner)
    a_local = pltpu.make_async_copy(fac, a_rows, a_sem.at[2])
    small_local = (
        pltpu.make_async_copy(wanted.at[0], wanted_v.at[x], i_sem.at[0, 3]),
        pltpu.make_async_copy(slots, slots_v.at[x], i_sem.at[1, 3]),
        pltpu.make_async_copy(cabs_hbm, cabs, o_sem.at[0]),
        pltpu.make_async_copy(coupling_hbm, coupling, o_sem.at[1]),
    )

    for g in range(CHUNKS):
        own_local(g).start()
    a_local.start()
    for cp in small_local:
        cp.start()
    lane = lax.broadcasted_iota(jnp.int32, (8, 16), 1)
    tile = jnp.zeros((8, 16), F32)
    for k in range(16):
        tile = jnp.where(lane == k, own_energy[k].astype(F32), tile)
    ens_v[y, x] = tile

    pl.semaphore_wait(barrier, len(greeted))

    @pl.when(c == 0)
    def _():
        start(own_first(0))
        start(own_second(0))

    @pl.when(c == 1)
    def _():
        start(own_second(0))
        start(own_first(0))

    a_partner.start()
    for cp in ints_copies() + ens_copies_x():
        cp.start()

    def step(t, carry):
        @pl.when(t < CHUNKS)
        def _():
            z_wait(t, 0)
            z_forward(t, 0).start()
            z_wait(t, 1)
            z_forward(t, 1).start()

        @pl.when(c == 0)
        def _():
            @pl.when(t == 0)
            def _():
                start(own_first(1))

            @pl.when(t < CHUNKS - 1)
            def _():
                start(own_second(t + 1))

            @pl.when(t < CHUNKS - 2)
            def _():
                start(own_first(t + 2))

        @pl.when(c == 1)
        def _():
            @pl.when(t == 0)
            def _():
                start(own_second(1))

            @pl.when(t < CHUNKS - 1)
            def _():
                start(own_first(t + 1))

            @pl.when(t < CHUNKS - 2)
            def _():
                start(own_second(t + 2))

        def send_rest(g):
            for i in (0, 2, 1):
                x_wait(g, i)
                y_start(g, i)
            to_partner(g, y).start()

        @pl.when((t == 1) | ((t >= 3) & (t < CHUNKS)))
        def _():
            send_rest(jnp.maximum(t - 2, 0))

        @pl.when((t == 0) | ((t >= 2) & (t < CHUNKS + 1)))
        def _():
            g = jnp.maximum(t - 1, 0)

            @pl.when(t == 0)
            def _():
                a_partner.wait_recv()
                a_local.wait()
                pltpu.make_async_copy(b_v.at[0], b_v.at[0], l_sem).wait()

            z_wait(g, 2)

            def fit(q):
                rows = pl.ds(pl.multiple_of(q * QROWS, QROWS), QROWS)
                acc = jnp.dot(a_v[rows, :], b_v[g], preferred_element_type=F32)
                return acc.T.astype(BF16)

            cols[col_at(c, y, g) + x] = fit(x)

            def fit_send(j, carry):
                i = jnp.where(j < 2, 1 - j, 2)
                q = (x + 3 - i) % 4
                f_v[g, q] = fit(q)
                x_copy(g, i).start()

                @pl.when(j == 0)
                def _():
                    y_start(g, 3)

                return carry

            lax.fori_loop(0, 3, fit_send, 0)

        @pl.when(t == CHUNKS)
        def _():
            send_rest(CHUNKS - 2)

        @pl.when((t >= 3) & (t < CHUNKS + 3))
        def _():
            g = t - 3
            for j, i in ((0, 3), (2, 0), (3, 2), (1, 1)):
                y_wait(g, j)
                y_forward(g, i).start()
            y_wait(g, 4)
            y_wait(g, 5)
            to_partner(g, ym).start()
            to_partner(g, yp).start()

        @pl.when(t == CHUNKS)
        def _():
            send_rest(CHUNKS - 1)

        @pl.when(t >= 4)
        def _():
            y_wait(t - 4, 6)
            to_partner(t - 4, yo).start()

        @pl.when(t == 2)
        def _():
            for cp in ints_copies() + ens_copies_x():
                cp.wait()
            for cp in small_local:
                cp.wait()
            for cp in ens_copies_y():
                cp.start()

        @pl.when(t == 6)
        def _():
            for cp in ens_copies_y():
                cp.wait()
            to_smem = (
                pltpu.make_async_copy(wanted_v, wanted_s, i_sem.at[2, 3]),
                pltpu.make_async_copy(slots_v, slots_s, i_sem.at[3, 3]),
                pltpu.make_async_copy(ens_v, ens_s, e_sem.at[1, 6]),
            )
            for cp in to_smem:
                cp.start()
            for cp in to_smem:
                cp.wait()

        return carry

    lax.fori_loop(0, CHUNKS + 4, step, 0)

    def sent(ref, sem):
        remote(ref, ref, sem, pr, me_partner).wait_send()

    remote(b_v, b_v, send_sem.at[3], pr, me_partner).wait_recv()
    sent(b_v.at[pl.ds(0, 7)], send_sem.at[0])
    sent(f_v.at[pl.ds(0, 6)], send_sem.at[1])
    sent(b_v.at[pl.ds(0, 6)], send_sem.at[2])
    sent(b_v, send_sem.at[3])
    a_partner.wait_send()

    def orbital(xo, position):
        k = slots_s[xo, 0, position]
        s = k >> 3
        t = wanted_s[xo, k & 7, s]
        return ((t >> 3) << 7) + ((s & 3) << 5) + ((t & 7) << 2) + (s >> 2)

    def pairs(half, first, steps=(0, 2)):
        def some(j, carry):
            done = []
            for slot in range(8):
                second = 2 * j + slot // 4
                xo, zz = (first, second) if half == 0 else (second, first)
                n = (2 * zz + c) * 8 + half * 4 + slot % 4
                left = cols[orbital(xo, 2 * n)]
                right = cols[orbital(xo, 2 * n + 1)]
                e = lax.dot_general(left, right, (((1,), (1,)), ((), ())), preferred_element_type=F32)
                done.append((e * SCALE).astype(BF16))
            for slot in range(8):
                part[half, first, j * 8 + slot] = done[slot]
            return carry

        lax.fori_loop(*steps, some, 0)

    def ring(half, d):
        if half == 0:
            at = (x + d) % 4
            return at, dev(z, c, at, y)
        at = (z + d) % 4
        return at, dev(at, c, x, y)

    def far_copy(half, i):
        far, _ = ring(half, 2)
        _, to = ring(half, 3 if i == 0 else 1)
        return remote(part.at[half, far, pl.ds(8 * i, 8)], rs_far.at[half, i], send_sem.at[4], r_sem.at[0, half, i], to)

    def near_copy(half, i, summed_part):
        at, to = ring(half, 3 if i == 0 else 1)
        first = 8 * i if summed_part else 8 - 8 * i
        j = 2 * i + (1 if summed_part else 0)
        rows = pl.ds(first, 8)
        return remote(part.at[half, at, rows], rs_near.at[half, i, rows], send_sem.at[4], r_sem.at[1, half, j], to)

    def combine(half, i):
        at, _ = ring(half, 3 if i == 0 else 1)
        far_copy(half, i).wait_recv()

        def add(k, carry):
            part[half, at, 8 * i + k] = (part[half, at, 8 * i + k].astype(F32) + rs_far[half, i, k].astype(F32)).astype(BF16)
            return carry

        lax.fori_loop(0, 8, add, 0, unroll=2)

    def rs2_copy(half, d):
        there, to = ring(1 - half, d)
        return remote(summed.at[half, pl.ds(there * 4, 4)], rs2.at[half, d - 1], send_sem.at[5], r_sem.at[2, half, 0], to)

    last = None
    for i in (0, 1):
        for half in (0, 1):
            pairs(half, ring(half, 2)[0], (i, i + 1))
            if last is not None:
                last.start()
            last = far_copy(half, i)
    last.start()
    for i, d in ((0, 3), (1, 1)):
        pairs(0, ring(0, d)[0])
        pairs(1, ring(1, d)[0])
        near_copy(0, i, False).start()
        near_copy(1, i, False).start()
    pairs(0, x)
    pairs(1, z)
    for half in (0, 1):
        for i in (0, 1):
            combine(half, i)
            near_copy(half, i, True).start()

    live = count[0]

    def energy(position):
        k = slots_s[x, 0, position]
        s = k >> 3
        return ens_s[s & 3, s >> 2, 0, wanted_s[x, k & 7, s]]

    for slot in range(8):
        n = f * 8 + slot
        denom = cabs[...] - (energy(2 * n) + energy(2 * n + 1))
        rec_v[slot] = jnp.where(n < live, 1.0 / denom, 0.0)

    for half in (0, 1):
        me_at = x if half == 0 else z
        for i in (0, 1):
            near_copy(half, i, False).wait_recv()
            near_copy(half, i, True).wait_recv()

        def add(i, carry):
            total = part[half, me_at, i].astype(F32)
            for d in (0, 1):
                total = total + rs_near[half, d, i].astype(F32)
            summed[half, i] = total.astype(BF16)
            return carry

        lax.fori_loop(0, 16, add, 0, unroll=2)
        for d in (2, 1, 3):
            rs2_copy(half, d).start()

    for half in (0, 1):
        me_at = z if half == 0 else x
        remote(rs2.at[half], rs2.at[half], send_sem.at[5], r_sem.at[2, half, 0], me_partner).wait_recv()

        for i in range(4):
            total = summed[half, me_at * 4 + i].astype(F32)
            for d in (0, 1, 2):
                total = total + rs2[half, d, i].astype(F32)
            exchange = total.astype(BF16)
            slot = half * 4 + i
            for at in range(0, 1024, 256):
                at = pl.ds(at, 256)
                weighted = jnp.dot(exchange, coupling[:, at], preferred_element_type=F32)
                out[0, slot, :, at] = (weighted * rec_v[slot, :, at]).astype(BF16)

    sent(b_v.at[pl.ds(0, 3)], send_sem.at[4])
    sent(rs2, send_sem.at[5])


def on_device(fac, tri, send_map, pair_slots, pair_count, orbital_energy, cabs_energy, coupling):
    dma = pltpu.SemaphoreType.DMA
    hbm = pl.BlockSpec(memory_space=pltpu.HBM)
    vmem = pl.BlockSpec(memory_space=pltpu.VMEM)
    smem = pl.BlockSpec(memory_space=pltpu.SMEM)
    return pl.pallas_call(
        fused_kernel,
        out_shape=jax.ShapeDtypeStruct((1, 8, LANES, 1024), BF16),
        in_specs=[hbm, hbm, hbm, hbm, hbm, hbm, smem, smem],
        out_specs=vmem,
        scratch_shapes=[
            pltpu.VMEM((2 * PANEL, 4096), BF16),
            pltpu.VMEM((CHUNKS, 4096, LANES), BF16),
            pltpu.VMEM((CHUNKS, 4, LANES, QROWS), BF16),
            pltpu.VMEM((256, LANES, QROWS), BF16),
            pltpu.VMEM((2, 4, 16, LANES, LANES), BF16),
            pltpu.VMEM((2, 2, 8, LANES, LANES), BF16),
            pltpu.VMEM((2, 2, 16, LANES, LANES), BF16),
            pltpu.VMEM((2, 16, LANES, LANES), BF16),
            pltpu.VMEM((2, 3, 4, LANES, LANES), BF16),
            pltpu.VMEM((4, 8, 16), jnp.int32),
            pltpu.VMEM((4, 1, LANES), jnp.int32),
            pltpu.VMEM((4, 4, 8, 16), F32),
            pltpu.SMEM((4, 8, 16), jnp.int32),
            pltpu.SMEM((4, 1, LANES), jnp.int32),
            pltpu.SMEM((4, 4, 8, 16), F32),
            pltpu.VMEM((8, 1, 1024), F32),
            pltpu.VMEM((1, 1024), F32),
            pltpu.VMEM((LANES, 1024), BF16),
            dma((6,)),
            dma((3,)),
            dma((CHUNKS, 3)),
            dma((CHUNKS, 3)),
            dma((CHUNKS, 7)),
            dma,
            dma((4, 4)),
            dma((2, 7)),
            dma((3, 2, 4)),
            dma,
            dma((2,)),
        ],
        compiler_params=pltpu.CompilerParams(
            collective_id=0, has_side_effects=True, vmem_limit_bytes=VMEM_LIMIT
        ),
        name="fit_exchange",
    )(
        *(
            pltpu.with_memory_space_constraint(a, pltpu.HBM)
            for a in (fac, tri, jnp.swapaxes(send_map, 1, 2), pair_slots, cabs_energy.reshape(1, 1024), coupling)
        ),
        pltpu.with_memory_space_constraint(orbital_energy, pltpu.HBM),
        pair_count,
    )


def solution(mesh):
    in_specs = (
        P("fit", None),
        P("fit", "pair"),
        P("pair", None, None),
        P("pair", None),
        P("pair"),
        P("pair"),
        P(),
        P(),
    )
    return jax.shard_map(
        on_device, mesh=mesh, in_specs=in_specs, out_specs=P("pair", "fit", None, None), check_vma=False
    )
```
